128 devices in a mesh: slab: 16 (over z, y), sub: 8 (over x, core).
Axes of the slice: x: 4, y: 4, z: 4, core: 2. Of those that a mesh axis runs over, the one named last changes fastest.
Arguments:
- velocity: float32 [65536, 3, 128], P(('slab', 'sub')), may hold values from -6 to 6
- weight: float32 [65536, 128], P(('slab', 'sub')), may hold values from 0.2 to 2
- offset: int32 [65536, 128], P(('slab', 'sub')), may hold values from 0 to 127
- owner: int32 [65536, 1], P(('slab', 'sub')), may hold values from 0 to 127; in each aligned block of 512 rows (0 to 511, 512 to 1023, ...) at most 8 rows name the same one
- brick: int32 [65536, 1], P(('slab', 'sub')), may hold values from 0 to 4095
- flags: int32 [128, 512, 1024], P('slab', 'sub'), may hold values from 0 to 2, as said below
Outputs:
- updated: float32 [65536, 3, 128], P(('slab', 'sub'))
- pressure: float32 [128, 512, 1024], P('slab', 'sub')
- solved_face_velocity: float32 [3, 128, 512, 1024], P(None, 'slab', 'sub')
The draws below stay inside these ranges and needn't reach their ends.
Inputs may be any that keep to these rules, and one draw needn't show every extreme that they name: Among the blocks of one device, at most 8 name the same owner. `flags`: 0 air, 1 liquid, 2 solid.
All inputs are finite; a program needn't handle non-finite values.
Results may differ from the reference program's by a relative error of at most 0.000075.
Values sent between devices are 32-bit elements; how exact they have to be, the bound alone decides.
No kernel may reach another device: no remote copies, remote signals or barrier semaphores. Data moves between devices by JAX's collectives and lax.ppermute only.
A program may use at most 128 MiB of HBM per device.

```python
import math
import jax
import jax.numpy as jnp
import numpy as np
from jax import lax

PB = 128
BC = 128
ITERS = 3
CX = 8
CY = 64
NZ = 1024
BLK_DEV = 512
NX = 128
NY = 512
BLOCKS = 65536
BRICKS_DEV = 4096
CAP = 8
N_SLAB = 16
N_SUB = 8
DEVICES = 128


def draw_flags(key, part):
    level = jax.random.randint(jax.random.fold_in(key, 7), (NX, NY, NZ), 0, 10)
    return jnp.where(level < 6, 1, jnp.where(level < 9, 0, 2)).astype(jnp.int32)


def place_ends(drawn, stream_key, low, top_value):
    shape = drawn.shape
    spot = [jax.random.randint(jax.random.fold_in(stream_key, axis), (), 0, shape[axis]) for axis in range(len(shape))]
    drawn = drawn.at[tuple(spot)].set(low)
    longest = shape.index(max(shape))
    spot[longest] = (spot[longest] + 1) % shape[longest]
    return drawn.at[tuple(spot)].set(top_value)


def block_scale(rng, dims, cuts, smallest, high):
    loudness, own = 1.0, jax.random.fold_in(rng, 6)
    for dim, blocks in cuts:
        heights = jnp.exp(jax.random.uniform(jax.random.fold_in(own, dim), (blocks,), jnp.float32, smallest / len(cuts), high / len(cuts)))
        loudness = loudness * jnp.repeat(heights, dims[dim] // blocks).reshape([-1 if axis == dim else 1 for axis in range(len(dims))])
    return loudness


def routed_block(own_key, own, number, rows, count, top, reach, lean):
    order = jax.random.permutation(own_key, count)
    heavy_load, usual = shares(count, rows * top, reach, lean, True), shares(count, rows * top, reach, lean, False)
    places = jnp.arange(count)

    def named(sizes, offset_by):
        used = int((sizes > 0).sum())
        fixed = max(1, used // 4)
        passed = fixed + (places - fixed + offset_by * (used - fixed)) % max(1, count - fixed)
        return jnp.zeros((count,), jnp.int32).at[order[jnp.where(places < fixed, places, passed)]].set(jnp.asarray(sizes, jnp.int32))

    sizes = jnp.where(number % 4 == 0, named(heavy_load, number // 4), named(usual, number - number // 4 - 1))
    mixed = jax.random.permutation(jax.random.fold_in(own, 3), count)
    donor, taker = mixed[0:count // 2 * 2:2], mixed[1:count // 2 * 2:2]
    slack = jnp.minimum(sizes[donor] - 1, reach - sizes[taker]) // 2
    slack = jnp.where((donor == order[0]) | (taker == order[0]) | (sizes[taker] == 0), 0, jnp.maximum(slack, 0))
    passed = jax.random.randint(jax.random.fold_in(own, 4), (count // 2,), 0, 1 << 20) % (slack + 1)
    sizes = sizes.at[donor].add(-passed).at[taker].add(passed)
    labels = jnp.searchsorted(jnp.cumsum(sizes), jnp.arange(rows * top), side="right").astype(jnp.int32)
    listing = labels.reshape(top, rows).T
    listing = listing[jax.random.permutation(jax.random.fold_in(own, 1), rows)]
    offset_by = jax.random.randint(jax.random.fold_in(own, 2), (rows, 1), 0, top)
    return jnp.take_along_axis(listing, (jnp.arange(top)[None, :] + offset_by) % top, axis=1)


def shares(number_of, total, limit, lean, full):
    weights = [(1 << 20) // math.isqrt(grade ** lean) + 1 for grade in range(1, number_of + 1)]
    largest = limit if full else min(limit, max(-(-total // number_of), total * weights[0] // sum(weights)))
    least = 1 if total - largest >= number_of - 1 else 0
    given, rest = [largest] + [least] * (number_of - 1), total - largest - least * (number_of - 1)
    while rest > 0:
        free = [i for i in range(1, number_of) if given[i] < largest] or [i for i in range(1, number_of) if given[i] < limit]
        whole, left = sum([weights[i] for i in free]), rest
        for i in free:
            addition = min(limit - given[i], max(1, left * weights[i] // whole), rest)
            given[i] = given[i] + addition
            rest = rest - addition
    return np.array(given)


def bell_draw(own_key, dims, scale, limit, cuts=(), held_as=jnp.bfloat16):
    drawn = scale * jax.random.normal(own_key, dims, jnp.float32)
    if cuts:
        drawn = drawn * block_scale(own_key, dims, cuts, -0.22, 0.18)
    return jnp.clip(drawn, -limit, limit).astype(held_as)


def setup_inputs(seed: int = 0) -> dict:
    streams_of = jax.random.split(jax.random.key(seed), 7)
    velocity = bell_draw(streams_of[0], (BLOCKS, 3, PB), 1.0, 6.0, ((0, 128),), jnp.float32)
    weight = jnp.clip(jnp.exp(math.log(2.0) - 2.3025851 * jax.random.uniform(streams_of[1], (BLOCKS, PB), jnp.float32) ** block_scale(streams_of[1], (BLOCKS, PB), ((0, 128),), -0.2, 0.2)), 0.2, 2.0)
    offset = place_ends(jax.random.randint(streams_of[2], (BLOCKS, PB), 0, BC), jax.random.fold_in(streams_of[2], 1), 0, BC - 1).astype(jnp.int32)
    owner_keys = jax.random.split(jax.random.fold_in(streams_of[3], 1), BLOCKS // BLK_DEV)
    owner_turns = jax.random.permutation(jax.random.fold_in(streams_of[3], 3), BLOCKS // BLK_DEV)
    owner = jax.vmap(lambda own, number: routed_block(jax.random.fold_in(streams_of[3], 2), own, number, BLK_DEV, DEVICES, 1, CAP, 2))(owner_keys, owner_turns).reshape((BLOCKS, 1))
    brick = place_ends(jax.random.randint(streams_of[4], (BLOCKS, 1), 0, BRICKS_DEV), jax.random.fold_in(streams_of[4], 1), 0, BRICKS_DEV - 1).astype(jnp.int32)
    flags = draw_flags(jax.random.fold_in(streams_of[6], 71), 0)
    return {"velocity": velocity, "weight": weight, "offset": offset, "owner": owner, "brick": brick, "flags": flags}


step_size = 0.15


def following(field, axis):
    edge = jnp.zeros_like(lax.slice_in_dim(field, 0, 1, axis=axis))
    return jnp.concatenate([lax.slice_in_dim(field, 1, field.shape[axis], axis=axis), edge], axis)


def preceding(field, axis):
    edge = jnp.zeros_like(lax.slice_in_dim(field, 0, 1, axis=axis))
    return jnp.concatenate([edge, lax.slice_in_dim(field, 0, field.shape[axis] - 1, axis=axis)], axis)


def reference(velocity, weight, offset, owner, brick, flags):
    target = owner[:, 0].astype(jnp.int32) * BRICKS_DEV + brick[:, 0].astype(jnp.int32)
    cell_index = (target[:, None] * BC + offset.astype(jnp.int32)).reshape(-1)
    loaded = jnp.concatenate([velocity * weight[:, None, :], weight[:, None, :]], 1)
    loaded = jnp.transpose(loaded, (0, 2, 1)).reshape(-1, 4)
    totals = jax.ops.segment_sum(loaded, cell_index, num_segments=DEVICES * BRICKS_DEV * BC)
    totals = totals.reshape(N_SLAB, N_SUB, CX, CY, NZ, 4).transpose(5, 0, 2, 1, 3, 4).reshape(4, NX, NY, NZ)
    metric = totals[3] + 1.0
    guess = totals[:3] / metric
    open_cell = (flags != 2).astype(jnp.float32)
    liquid = (flags == 1).astype(jnp.float32)
    faces_open = jnp.stack([open_cell * following(open_cell, axis) for axis in range(3)])
    solved_face_velocity = faces_open * guess
    pressure = jnp.zeros_like(metric)
    for sweep in range(ITERS):
        spread = solved_face_velocity[0] - preceding(solved_face_velocity[0], 0)
        spread = spread + (solved_face_velocity[1] - preceding(solved_face_velocity[1], 1))
        spread = spread + (solved_face_velocity[2] - preceding(solved_face_velocity[2], 2))
        pressure = liquid * jnp.maximum(pressure - step_size * spread, 0.0)
        push = jnp.stack([pressure - following(pressure, axis) for axis in range(3)])
        solved_face_velocity = faces_open * (guess + push / metric)
    change = solved_face_velocity - guess
    flat = change.reshape(3, N_SLAB, CX, N_SUB, CY, NZ).transpose(1, 3, 2, 4, 5, 0).reshape(-1, 3)
    picked = flat[cell_index].reshape(BLOCKS, PB, 3).transpose(0, 2, 1)
    return velocity + picked, pressure, solved_face_velocity
```

```python
import functools
import jax
import jax.numpy as jnp
from jax import lax
from jax.experimental import pallas as pl
from jax.experimental.pallas import tpu as pltpu
from jax.sharding import PartitionSpec as P

F32 = jnp.float32
BF16 = jnp.bfloat16
I32 = jnp.int32
LANES = 128
CHUNK = 33
COLUMN = 33
MIB = 1 << 20


def vmem():
    return pl.BlockSpec(memory_space=pltpu.VMEM)


def smem():
    return pl.BlockSpec(memory_space=pltpu.SMEM)


def call(kernel, ins, outs, shapes, scratch=(), limit=16, flops=2_000_000, **kw):
    return pl.pallas_call(
        kernel,
        in_specs=ins,
        out_specs=outs,
        out_shape=shapes,
        scratch_shapes=list(scratch),
        compiler_params=pltpu.CompilerParams(vmem_limit_bytes=limit * MIB),
        cost_estimate=pl.CostEstimate(flops=flops, bytes_accessed=1 << 20, transcendentals=0),
        **kw,
    )


def two_parts(x):
    high = x.astype(BF16).astype(F32)
    return high, x - high


def one_hot(offsets, cells):
    return jnp.where(jnp.broadcast_to(offsets, cells.shape) == cells, 1.0, 0.0).astype(BF16)


def splat_kernel(vel, weight, offset, owner, brick, out, place, parts, names, count):
    blocks = weight.shape[0]
    devices = names.shape[0]
    out[...] = jnp.zeros_like(out)
    names[...] = jnp.full(names.shape, 4096.0, F32)

    def clear(d, carry):
        count[d] = 0
        return carry

    lax.fori_loop(0, devices, clear, 0, unroll=8)

    def load(g, carry):
        rows = pl.ds(pl.multiple_of(g * 8, 8), 8)
        w = weight[rows, :]
        base = pl.multiple_of(g * 128, 128)
        for c in range(4):
            high, low = two_parts(vel[c, rows, :] * w if c < 3 else w)
            parts[pl.ds(base + c, 8, stride=16), :] = high
            parts[pl.ds(base + 8 + c, 8, stride=16), :] = low
        return carry

    lax.fori_loop(0, blocks // 8, load, 0, unroll=2)
    cells = lax.broadcasted_iota(I32, (LANES, LANES), 0)
    lane = lax.broadcasted_iota(I32, (1, LANES), 1)
    many = 8

    def step(g, carry):
        base = pl.multiple_of(g * many, many)
        offs = offset[pl.ds(base, many), :]
        sums = []
        for j in range(many):
            hot = one_hot(offs[j : j + 1, :], cells)
            lhs = parts[pl.ds(pl.multiple_of(base * 16, 128) + 16 * j, 16), :].astype(BF16)
            r = lax.dot_general(lhs, hot, (((1,), (1,)), ((), ())), preferred_element_type=F32)
            sums.append(r[0:8] + r[8:16])
        for j in range(many):
            d = owner[base + j]
            slot = count[d]
            count[d] = slot + 1
            place[base + j] = d * 8 + slot
            out[pl.ds(d * CHUNK + slot * 4, 4), :] = sums[j][0:4]
            b = brick[base + j]
            old = names[pl.ds(d, 1), :]
            names[pl.ds(d, 1), :] = jnp.where(lane == slot, jnp.full((1, LANES), b, I32).astype(F32), old)
        return carry

    lax.fori_loop(0, blocks // many, step, 0)
    out[pl.ds(32, devices, stride=CHUNK), :] = names[...]


def splat(vel, weight, offset, owner, brick, devices):
    blocks = weight.shape[0]
    return call(
        splat_kernel,
        [vmem()] * 3 + [smem()] * 2,
        [vmem(), smem()],
        [jax.ShapeDtypeStruct((devices * CHUNK, LANES), F32), jax.ShapeDtypeStruct((blocks,), I32)],
        [pltpu.VMEM((blocks * 16, LANES), F32), pltpu.VMEM((devices, LANES), F32), pltpu.SMEM((devices,), I32)],
    )(vel, weight, offset, owner, brick)


def pick_kernel(ret, vel, offset, place, out, parts, sums):
    blocks = offset.shape[0]
    cells = lax.broadcasted_iota(I32, (LANES, LANES), 0)
    many = 8

    def gather(g, carry):
        base = pl.multiple_of(g * 8, 8)
        for j in range(8):
            x = ret[pl.ds(place[base + j] * 3, 3), :]
            high, low = two_parts(x)
            at = pl.multiple_of(base * 16, 128) + 16 * j
            parts[pl.ds(at, 3), :] = high
            parts[pl.ds(at + 8, 3), :] = low
        return carry

    lax.fori_loop(0, blocks // 8, gather, 0)

    def step(g, carry):
        base = pl.multiple_of(g * many, many)
        offs = offset[pl.ds(base, many), :]
        for j in range(many):
            hot = one_hot(offs[j : j + 1, :], cells)
            lhs = parts[pl.ds(pl.multiple_of(base * 16, 128) + 16 * j, 16), :].astype(BF16)
            r = lax.dot_general(lhs, hot, (((1,), (0,)), ((), ())), preferred_element_type=F32)
            sums[pl.ds(pl.multiple_of(base * 8, 64) + 8 * j, 8), :] = r[0:8] + r[8:16]
        return carry

    lax.fori_loop(0, blocks // many, step, 0)

    def add(g, carry):
        rows = pl.ds(pl.multiple_of(g * 8, 8), 8)
        for c in range(3):
            out[c, rows, :] = vel[c, rows, :] + sums[pl.ds(pl.multiple_of(g * 64, 64) + c, 8, stride=8), :]
        return carry

    lax.fori_loop(0, blocks // 8, add, 0, unroll=4)


def pick(ret, vel, offset, place):
    blocks = offset.shape[0]
    return call(
        pick_kernel,
        [vmem()] * 3 + [smem()],
        vmem(),
        jax.ShapeDtypeStruct((3, blocks, LANES), F32),
        [pltpu.VMEM((blocks * 16, LANES), F32), pltpu.VMEM((blocks * 8, LANES), F32)],
    )(ret, vel, offset, place)


def scatter_kernel(arr, names, tot, first, last):
    xs, ys = first.shape[0] // 96, 64
    per = 8 * CHUNK

    def clear(g, carry):
        tot[pl.ds(pl.multiple_of(g * 8, 8), 8), :] = jnp.zeros((8, LANES), F32)
        return carry

    lax.fori_loop(0, tot.shape[0] // 8, clear, 0, unroll=16)

    def step(g, carry):
        base = pl.multiple_of(g * per, 8)
        for k in range(64):
            b = names[g * 64 + k]
            row = (b >> 3) * COLUMN + (b & 7) * 4
            at = pl.ds(row, 4)
            tot[at, :] = tot[at, :] + arr[pl.ds(base + (k // 8) * CHUNK + (k % 8) * 4, 4), :]
        return carry

    lax.fori_loop(0, arr.shape[0] // per, step, 0)
    for x in range(xs):
        for r in range(3):
            first[pl.ds(x * 96 + r * 32, 32), :] = tot[pl.ds((x * ys + r) * COLUMN, 32), :]
            last[pl.ds(x * 96 + r * 32, 32), :] = tot[pl.ds((x * ys + ys - 3 + r) * COLUMN, 32), :]


def scatter(arr, names, xs, ys):
    rows = xs * ys * COLUMN + 8
    halo = jax.ShapeDtypeStruct((xs * 96, LANES), F32)
    return call(
        scatter_kernel,
        [vmem(), smem()],
        [vmem()] * 3,
        [jax.ShapeDtypeStruct((rows, LANES), F32), halo, halo],
    )(arr, names)
ROWS = 72
FACE_X, FACE_Y, FACE_Z, LIQUID = 1, 2, 4, 8
STEP = 0.15


def strip(z):
    return pl.ds(z * LANES, LANES)


def lanes():
    return lax.broadcasted_iota(I32, (ROWS, LANES), 1)


def before_y(a):
    return pltpu.roll(a, 1, 0)


def after_y(a):
    return pltpu.roll(a, ROWS - 1, 0)


def before_z(strips):
    lane = lanes()
    rolled = [pltpu.roll(a, 1, 1) for a in strips]
    return [jnp.where(lane == 0, rolled[z - 1], rolled[z]) for z in range(len(strips))]


def after_z(strips):
    lane = lanes()
    rolled = [pltpu.roll(a, LANES - 1, 1) for a in strips]
    last = len(strips) - 1
    return [jnp.where(lane == LANES - 1, rolled[z + 1 if z < last else 0], rolled[z]) for z in range(len(strips))]


def strips_of(ref, index, count):
    return [ref[(*index, slice(None), strip(z))] for z in range(count)]


def code_kernel(flags, tile, beyond, code):
    xs, zs = code.shape[0], code.shape[2] // LANES

    def encoded(x):
        def one(z):
            f = flags[x, :, strip(z)]
            return jnp.concatenate([jnp.where(f == 2, 0, f + 1), tile[x, :, strip(z)]], 0)

        return [one(z) for z in range(zs)]

    def layer(x, e, e_next):
        o = [jnp.minimum(a, 1) for a in e]
        o_z = after_z(o)
        lane = lanes()
        o_z[-1] = jnp.where(lane == LANES - 1, 0, o_z[-1])
        for z in range(zs):
            c = o[z] & jnp.minimum(e_next[z], 1)
            c = c | ((o[z] & after_y(o[z])) << 1) | ((o[z] & o_z[z]) << 2)
            code[x, :, strip(z)] = c | jnp.where(e[z] == 2, LIQUID, 0)

    def step(x, carry):
        layer(x, encoded(x), encoded(x + 1))
        return carry

    lax.fori_loop(0, xs - 1, step, 0)
    layer(xs - 1, encoded(xs - 1), strips_of(beyond, (), zs))


def make_code(flags, tile, beyond):
    xs, _, nz = flags.shape
    return call(
        code_kernel, [vmem()] * 3, vmem(), jax.ShapeDtypeStruct((xs, ROWS, nz), I32)
    )(flags, tile, beyond)


def partial_spread(v, x, zs):
    vx, vy, vz = (strips_of(v, (a, x), zs) for a in range(3))
    vz_before = before_z(vz)
    return [vx[z] + (vy[z] - before_y(vy[z])) + (vz[z] - vz_before[z]) for z in range(zs)]


def send_layers(v, to_next, to_prior, xs, zs):
    for z, s in enumerate(partial_spread(v, 0, zs)):
        to_prior[:, strip(z)] = s
    to_next[...] = v[0, xs - 1]


def fields_kernel(tot, after, prior, code, guess, inverse, v, to_next, to_prior, edge):
    xs, ys, zs = code.shape[0], ROWS - 8, code.shape[2] // LANES
    for x in range(xs):
        edge[pl.ds(x * 256, 96), :] = after[pl.ds(x * 96, 96), :]
        edge[pl.ds(x * 256 + 96, 64), :] = jnp.zeros((64, LANES), F32)
        edge[pl.ds(x * 256 + 160, 96), :] = prior[pl.ds(x * 96, 96), :]

    def step(x, carry):
        for z in range(zs):
            def read(c):
                rows = [
                    tot[pl.ds((x * ys + y * 8) * COLUMN + z * 4 + c, 8, stride=COLUMN), :]
                    for y in range(ys // 8)
                ]
                rows.append(edge[pl.ds(x * 256 + z * 4 + c, 8, stride=32), :])
                return jnp.concatenate(rows, 0)

            r = 1.0 / (read(3) + 1.0)
            inverse[x, :, strip(z)] = r
            bits = code[x, :, strip(z)]
            for a in range(3):
                g = read(a) * r
                guess[a, x, :, strip(z)] = g
                v[a, x, :, strip(z)] = jnp.where(bits & (1 << a) != 0, g, 0.0)
        return carry

    lax.fori_loop(0, xs, step, 0)
    send_layers(v, to_next, to_prior, xs, zs)


def fields(tot, after, prior, code):
    xs, _, nz = code.shape
    one = jax.ShapeDtypeStruct((xs, ROWS, nz), F32)
    three = jax.ShapeDtypeStruct((3, xs, ROWS, nz), F32)
    layer = jax.ShapeDtypeStruct((ROWS, nz), F32)
    return call(
        fields_kernel,
        [vmem()] * 4,
        [vmem()] * 5,
        [three, one, three, layer, layer],
        [pltpu.VMEM((xs * 256, LANES), F32)],
    )(tot, after, prior, code)


def ascend(p_out, p_in, v, code, x, before, first, zs):
    spread = partial_spread(v, x, zs)
    for z in range(zs):
        s = spread[z] - before(z)
        old = -STEP * s if first else p_in[x, :, strip(z)] - STEP * s
        liquid = code[x, :, strip(z)] & LIQUID != 0
        p_out[x, :, strip(z)] = jnp.where(liquid, jnp.maximum(old, 0.0), 0.0)


def push(v_out, p, code, guess, inverse, x, after, zs):
    here = strips_of(p, (x,), zs)
    here_z = after_z(here)
    for z in range(zs):
        r = inverse[x, :, strip(z)]
        bits = code[x, :, strip(z)]
        beyond = (after(z), after_y(here[z]), here_z[z])
        for a in range(3):
            moved = guess[a, x, :, strip(z)] + (here[z] - beyond[a]) * r
            v_out[a, x, :, strip(z)] = jnp.where(bits & (1 << a) != 0, moved, 0.0)


def inner_kernel(first, p_in, v_in, code, guess, inverse, p, v):
    xs, zs = code.shape[0], code.shape[2] // LANES

    def up(x, carry):
        ascend(p, p_in, v_in, code, x, lambda z: v_in[0, x - 1, :, strip(z)], first, zs)
        return carry

    lax.fori_loop(1, xs, up, 0)

    def out(x, carry):
        push(v, p, code, guess, inverse, x, lambda z: p[x + 1, :, strip(z)], zs)
        return carry

    lax.fori_loop(1, xs - 1, out, 0)


def outer_kernel(first, before, spread, beyond, p8_in, p_in, v_in, code, guess, inverse, p, v, p8, to_next, to_prior):
    xs, zs = code.shape[0], code.shape[2] // LANES
    ascend(p, p_in, v_in, code, 0, lambda z: before[:, strip(z)], first, zs)
    for z in range(zs):
        s = spread[:, strip(z)] - v_in[0, xs - 1, :, strip(z)]
        old = -STEP * s if first else p8_in[:, strip(z)] - STEP * s
        p8[:, strip(z)] = jnp.where(beyond[:, strip(z)] == 2, jnp.maximum(old, 0.0), 0.0)
    push(v, p, code, guess, inverse, 0, lambda z: p[1, :, strip(z)], zs)
    push(v, p, code, guess, inverse, xs - 1, lambda z: p8[:, strip(z)], zs)
    send_layers(v, to_next, to_prior, xs, zs)


def inner(first, p, v, code, guess, inverse):
    shapes = [jax.ShapeDtypeStruct(a.shape, F32) for a in (p, v)]
    return call(
        functools.partial(inner_kernel, first),
        [vmem()] * 5,
        [vmem()] * 2,
        shapes,
        input_output_aliases={0: 0, 1: 1},
    )(p, v, code, guess, inverse)


def outer(first, before, spread, beyond, p8, p, v, code, guess, inverse):
    shapes = [jax.ShapeDtypeStruct(a.shape, F32) for a in (p, v, p8, p8, p8)]
    return call(
        functools.partial(outer_kernel, first),
        [vmem()] * 9,
        [vmem()] * 5,
        shapes,
        input_output_aliases={4: 0, 5: 1},
    )(before, spread, beyond, p8, p, v, code, guess, inverse)


def reply_kernel(v, guess, names, reply, change):
    xs, ys, zs = v.shape[1], ROWS - 8, v.shape[3] // LANES

    def turn(x, carry):
        for a in range(3):
            for z in range(zs):
                for y in range(ys // 8):
                    at = (a, x, slice(y * 8, y * 8 + 8), strip(z))
                    change[pl.ds((x * ys + y * 8) * COLUMN + z * 4 + a, 8, stride=COLUMN), :] = v[at] - guess[at]
        return carry

    lax.fori_loop(0, xs, turn, 0)

    def step(g, carry):
        base = pl.multiple_of(g * 192, 192)
        for k in range(64):
            b = names[g * 64 + k]
            reply[pl.ds(base + 3 * k, 3), :] = change[pl.ds((b >> 3) * COLUMN + (b & 7) * 4, 3), :]
        return carry

    lax.fori_loop(0, reply.shape[0] // 192, step, 0)


def make_reply(v, guess, names):
    xs = v.shape[1]
    return call(
        reply_kernel,
        [vmem()] * 2 + [smem()],
        vmem(),
        jax.ShapeDtypeStruct((names.shape[0] * 3, LANES), F32),
        [pltpu.VMEM((xs * (ROWS - 8) * COLUMN + 8, LANES), F32)],
    )(v, guess, names)


def shifted(block, axis, distance):
    devices = range(lax.axis_size(axis))
    return lax.ppermute(block, axis, [(i - distance, i) for i in devices if i - distance in devices])


ITERS = 3


def on_device(velocity, weight, offset, owner, brick, flags):
    devices = lax.axis_size("slab") * lax.axis_size("sub")
    xs, ys, nz = flags.shape
    both = ("slab", "sub")
    kinds = jnp.where(flags == 2, 0, flags + 1)
    later = shifted(kinds[:, :4], "sub", -1)
    prior = shifted(kinds[:, ys - 3 :], "sub", 1)
    tile = jnp.concatenate([later, jnp.zeros((xs, 1, nz), I32), prior], 1)
    beyond = shifted(jnp.concatenate([kinds[0], tile[0]], 0), "slab", -1)
    planes = velocity.transpose(1, 0, 2)
    outgoing, place = splat(planes, weight, offset, owner[:, 0], brick[:, 0], devices)
    arrived = lax.all_to_all(outgoing.reshape(devices, 1, CHUNK * LANES), both, 0, 0, tiled=True)
    code = make_code(flags, tile, beyond)
    names = arrived[:, 0, 32 * LANES : 32 * LANES + 8].astype(I32).reshape(-1)
    totals, first_rows, last_rows = scatter(arrived.reshape(devices * CHUNK, LANES), names, xs, ys)
    after = shifted(first_rows, "sub", -1)
    before = shifted(last_rows, "sub", 1)
    guess, inverse, v, to_next, to_prior = fields(totals, after, before, code)
    p = jnp.zeros((xs, ROWS, nz), F32)
    p8 = jnp.zeros((ROWS, nz), F32)
    for sweep in range(ITERS):
        from_prior = shifted(to_next, "slab", 1)
        from_next = shifted(to_prior, "slab", -1)
        p, v = inner(sweep == 0, p, v, code, guess, inverse)
        p, v, p8, to_next, to_prior = outer(
            sweep == 0, from_prior, from_next, beyond, p8, p, v, code, guess, inverse
        )
    reply = make_reply(v, guess, names)
    back = lax.all_to_all(reply.reshape(devices, 24, LANES), both, 0, 0, tiled=True)
    updated = pick(back.reshape(devices * 24, LANES), planes, offset, place)
    return updated.transpose(1, 0, 2), p[:, :ys], v[:, :, :ys]


def solution(mesh):
    return jax.shard_map(
        on_device,
        mesh=mesh,
        in_specs=(P(("slab", "sub")),) * 5 + (P("slab", "sub"),),
        out_specs=(P(("slab", "sub")), P("slab", "sub"), P(None, "slab", "sub")),
        check_vma=False,
    )
```

```python
import functools
import jax
import jax.numpy as jnp
from jax import lax
from jax.experimental import pallas as pl
from jax.experimental.pallas import tpu as pltpu
from jax.sharding import PartitionSpec as P

F32 = jnp.float32
BF16 = jnp.bfloat16
I32 = jnp.int32
LANES = 128
CHUNK = 33
COLUMN = 33
MIB = 1 << 20
GROUP = 64


def vmem():
    return pl.BlockSpec(memory_space=pltpu.VMEM)


def hbm():
    return pl.BlockSpec(memory_space=pltpu.HBM)


def smem():
    return pl.BlockSpec(memory_space=pltpu.SMEM)


def call(kernel, ins, outs, shapes, scratch=(), limit=3, micros=3, **kw):
    return pl.pallas_call(
        kernel,
        in_specs=ins,
        out_specs=outs,
        out_shape=shapes,
        scratch_shapes=list(scratch),
        compiler_params=pltpu.CompilerParams(vmem_limit_bytes=limit * MIB),
        cost_estimate=pl.CostEstimate(flops=micros * 100_000_000, bytes_accessed=1 << 20, transcendentals=0),
        **kw,
    )


def two_parts(x):
    high = x.astype(BF16).astype(F32)
    return high, x - high


def one_hot(offsets, cells):
    return jnp.where(jnp.broadcast_to(offsets, cells.shape) == cells, 1.0, 0.0).astype(BF16)


def splat_kernel(
    vel_hbm, weight_hbm, offset_hbm, owner_hbm, brick_hbm, out, place,
    vel, weight, offset, owner, brick, parts, names, count, sems
):
    pairs = ((vel_hbm, vel), (weight_hbm, weight), (offset_hbm, offset), (owner_hbm, owner), (brick_hbm, brick))
    copies = [pltpu.make_async_copy(a, b, sems.at[i]) for i, (a, b) in enumerate(pairs)]
    for copy in copies:
        copy.start()
    blocks = weight.shape[0]
    devices = names.shape[0]
    names[...] = jnp.full(names.shape, 4096.0, F32)

    def clear(g, carry):
        out[pl.ds(pl.multiple_of(g * 8, 8), 8), :] = jnp.zeros((8, LANES), F32)
        return carry

    lax.fori_loop(0, out.shape[0] // 8, clear, 0, unroll=16)

    def reset(d, carry):
        count[d] = 0
        return carry

    lax.fori_loop(0, devices, reset, 0, unroll=8)
    for copy in copies:
        copy.wait()

    def load(g, carry):
        for half in range(2):
            rows = pl.ds(pl.multiple_of(g * 16 + 8 * half, 8), 8)
            w = weight[rows, :]
            base = pl.multiple_of(g * 128, 128) + 4 * half
            for c in range(4):
                high, low = two_parts(vel[c, rows, :] * w if c < 3 else w)
                parts[pl.ds(base + c, 8, stride=16), :] = high
                parts[pl.ds(base + 8 + c, 8, stride=16), :] = low
        return carry

    lax.fori_loop(0, blocks // 16, load, 0, unroll=2)
    cells = lax.broadcasted_iota(I32, (LANES, LANES), 0)
    lane = lax.broadcasted_iota(I32, (1, LANES), 1)
    upper = lax.broadcasted_iota(I32, (16, LANES), 0) % 8 < 4

    def step(g, carry):
        base = pl.multiple_of(g * GROUP, GROUP)
        offs = offset[pl.ds(base, GROUP), :]
        sums = [None] * GROUP
        for t in range(GROUP // 16):
            for q in range(8):
                one, two = t * 16 + q, t * 16 + 8 + q
                hot = jnp.concatenate(
                    [one_hot(offs[one : one + 1, :], cells), one_hot(offs[two : two + 1, :], cells)], 1
                )
                x = parts[pl.ds(pl.multiple_of(base * 8, 8 * GROUP) + 128 * t + 16 * q, 16), :]
                lhs = jnp.concatenate([jnp.where(upper, x, 0.0), jnp.where(upper, 0.0, x)], 1).astype(BF16)
                r = lax.dot_general(lhs, hot, (((1,), (1,)), ((), ())), preferred_element_type=F32)
                r = r[0:8] + r[8:16]
                sums[one], sums[two] = r[0:4], r[4:8]
        for j in range(GROUP):
            d = owner[base + j]
            slot = count[d]
            count[d] = slot + 1
            place[base + j] = d * 8 + slot
            out[pl.ds(d * CHUNK + slot * 4, 4), :] = sums[j]
            b = brick[base + j]
            old = names[pl.ds(d, 1), :]
            names[pl.ds(d, 1), :] = jnp.where(lane == slot, jnp.full((1, LANES), b, I32).astype(F32), old)
        return carry

    lax.fori_loop(0, blocks // GROUP, step, 0)
    out[pl.ds(32, devices, stride=CHUNK), :] = names[...]


def splat(vel, weight, offset, owner, brick, devices):
    blocks = weight.shape[0]
    return call(
        splat_kernel,
        [hbm()] * 5,
        [vmem(), smem()],
        [jax.ShapeDtypeStruct((devices * CHUNK, LANES), F32), jax.ShapeDtypeStruct((blocks,), I32)],
        [
            pltpu.VMEM(vel.shape, F32),
            pltpu.VMEM(weight.shape, F32),
            pltpu.VMEM(offset.shape, I32),
            pltpu.SMEM((blocks,), I32),
            pltpu.SMEM((blocks,), I32),
            pltpu.VMEM((blocks * 8, LANES), F32),
            pltpu.VMEM((devices, LANES), F32),
            pltpu.SMEM((devices,), I32),
            pltpu.SemaphoreType.DMA((5,)),
        ],
        limit=60,
        micros=8,
    )(vel, weight, offset, owner, brick)


def pick_kernel(ret, vel, offset, place, out, parts, sums):
    blocks = offset.shape[0]
    cells = lax.broadcasted_iota(I32, (LANES, LANES), 0)
    upper = lax.broadcasted_iota(I32, (8, LANES), 0) < 4

    def gather(g, carry):
        base = pl.multiple_of(g * 16, 16)
        for j in range(16):
            high, low = two_parts(ret[pl.ds(place[base + j] * 3, 3), :])
            at = pl.multiple_of(base * 8, 128) + 16 * (j % 8) + 4 * (j // 8)
            parts[pl.ds(at, 3), :] = high
            parts[pl.ds(at + 8, 3), :] = low
        return carry

    lax.fori_loop(0, blocks // 16, gather, 0)

    def step(g, carry):
        base = pl.multiple_of(g * GROUP, GROUP)
        offs = offset[pl.ds(base, GROUP), :]
        for t in range(GROUP // 16):
            for q in range(8):
                one, two = t * 16 + q, t * 16 + 8 + q
                hot = jnp.concatenate(
                    [one_hot(offs[one : one + 1, :], cells), one_hot(offs[two : two + 1, :], cells)], 1
                )
                lhs = parts[pl.ds(pl.multiple_of(base * 8, 8 * GROUP) + 128 * t + 16 * q, 16), :].astype(BF16)
                r = lax.dot_general(lhs, hot, (((1,), (0,)), ((), ())), preferred_element_type=F32)
                r = r[0:8] + r[8:16]
                at = pl.multiple_of(base * 4, 4 * GROUP) + 64 * t + 8 * q
                sums[pl.ds(at, 8), :] = jnp.where(upper, r[:, :LANES], r[:, LANES:])
        return carry

    lax.fori_loop(0, blocks // GROUP, step, 0)

    def add(g, carry):
        for half in range(2):
            rows = pl.ds(pl.multiple_of(g * 16 + 8 * half, 8), 8)
            for c in range(3):
                change = sums[pl.ds(pl.multiple_of(g * 64, 64) + 4 * half + c, 8, stride=8), :]
                out[c, rows, :] = vel[c, rows, :] + change
        return carry

    lax.fori_loop(0, blocks // 16, add, 0, unroll=4)


def pick(ret, vel, offset, place):
    blocks = offset.shape[0]
    return call(
        pick_kernel,
        [vmem()] * 3 + [smem()],
        vmem(),
        jax.ShapeDtypeStruct((3, blocks, LANES), F32),
        [pltpu.VMEM((blocks * 8, LANES), F32), pltpu.VMEM((blocks * 4, LANES), F32)],
        limit=12,
        micros=6,
    )(ret, vel, offset, place)


def scatter_kernel(arr_hbm, names, tot, first, last, arr, sem):
    xs, ys = first.shape[0] // 96, 64
    per = 8 * CHUNK
    load = pltpu.make_async_copy(arr_hbm, arr, sem.at[0])
    load.start()

    def clear(g, carry):
        tot[pl.ds(pl.multiple_of(g * 8, 8), 8), :] = jnp.zeros((8, LANES), F32)
        return carry

    lax.fori_loop(0, tot.shape[0] // 8, clear, 0, unroll=16)
    load.wait()

    def step(g, carry):
        base = pl.multiple_of(g * per, 8)
        for k in range(64):
            b = names[g * 64 + k]
            row = (b >> 3) * COLUMN + (b & 7) * 4
            at = pl.ds(row, 4)
            tot[at, :] = tot[at, :] + arr[pl.ds(base + (k // 8) * CHUNK + (k % 8) * 4, 4), :]
        return carry

    lax.fori_loop(0, arr.shape[0] // per, step, 0)
    for x in range(xs):
        for r in range(3):
            first[pl.ds(x * 96 + r * 32, 32), :] = tot[pl.ds((x * ys + r) * COLUMN, 32), :]
            last[pl.ds(x * 96 + r * 32, 32), :] = tot[pl.ds((x * ys + ys - 3 + r) * COLUMN, 32), :]


def scatter(arr, names, xs, ys):
    rows = xs * ys * COLUMN + 8
    halo = jax.ShapeDtypeStruct((xs * 96, LANES), F32)
    return call(
        scatter_kernel,
        [hbm(), smem()],
        [vmem()] * 3,
        [jax.ShapeDtypeStruct((rows, LANES), F32), halo, halo],
        [pltpu.VMEM(arr.shape, F32), pltpu.SemaphoreType.DMA((1,))],
    )(arr, names)
ROWS = 72
FACE_X, FACE_Y, FACE_Z, LIQUID = 1, 2, 4, 8
STEP = 0.15


def strip(z):
    return pl.ds(z * LANES, LANES)


def lanes():
    return lax.broadcasted_iota(I32, (ROWS, LANES), 1)


def before_y(a):
    return pltpu.roll(a, 1, 0)


def after_y(a):
    return pltpu.roll(a, ROWS - 1, 0)


def before_z(strips):
    lane = lanes()
    rolled = [pltpu.roll(a, 1, 1) for a in strips]
    return [jnp.where(lane == 0, rolled[z - 1], rolled[z]) for z in range(len(strips))]


def after_z(strips):
    lane = lanes()
    rolled = [pltpu.roll(a, LANES - 1, 1) for a in strips]
    last = len(strips) - 1
    return [jnp.where(lane == LANES - 1, rolled[z + 1 if z < last else 0], rolled[z]) for z in range(len(strips))]


def strips_of(ref, index, count):
    return [ref[(*index, slice(None), strip(z))] for z in range(count)]


def code_kernel(flags, tile, beyond, code):
    xs, zs = code.shape[0], code.shape[2] // LANES

    def encoded(x):
        def one(z):
            f = flags[x, :, strip(z)]
            return jnp.concatenate([jnp.where(f == 2, 0, f + 1), tile[x, :, strip(z)]], 0)

        return [one(z) for z in range(zs)]

    def layer(x, e, e_next):
        o = [jnp.minimum(a, 1) for a in e]
        o_z = after_z(o)
        lane = lanes()
        o_z[-1] = jnp.where(lane == LANES - 1, 0, o_z[-1])
        for z in range(zs):
            c = o[z] & jnp.minimum(e_next[z], 1)
            c = c | ((o[z] & after_y(o[z])) << 1) | ((o[z] & o_z[z]) << 2)
            code[x, :, strip(z)] = c | jnp.where(e[z] == 2, LIQUID, 0)

    def step(x, carry):
        layer(x, encoded(x), encoded(x + 1))
        return carry

    lax.fori_loop(0, xs - 1, step, 0)
    layer(xs - 1, encoded(xs - 1), strips_of(beyond, (), zs))


def make_code(flags, tile, beyond):
    xs, _, nz = flags.shape
    return call(
        code_kernel, [vmem()] * 3, vmem(), jax.ShapeDtypeStruct((xs, ROWS, nz), I32)
    )(flags, tile, beyond)


def partial_spread(v, x, zs):
    vx, vy, vz = (strips_of(v, (a, x), zs) for a in range(3))
    vz_before = before_z(vz)
    return [vx[z] + (vy[z] - before_y(vy[z])) + (vz[z] - vz_before[z]) for z in range(zs)]


def send_layers(v, to_next, to_prior, xs, zs):
    for z, s in enumerate(partial_spread(v, 0, zs)):
        to_prior[:, strip(z)] = s
    to_next[...] = v[0, xs - 1]


def fill(read, code, guess, inverse, v, x, rows, z):
    at = (x, rows, strip(z))
    r = 1.0 / (read(3) + 1.0)
    inverse[at] = r
    bits = code[at]
    for a in range(3):
        g = read(a) * r
        guess[(a, *at)] = g
        v[(a, *at)] = jnp.where(bits & (1 << a) != 0, g, 0.0)


def fields_kernel(tot, code, guess, inverse, v):
    xs, ys, zs = code.shape[0], ROWS - 8, code.shape[2] // LANES

    def step(x, carry):
        for z in range(zs):
            for y in range(0, ys, 8):
                start = (x * ys + y) * COLUMN + z * 4
                read = lambda c: tot[pl.ds(start + c, 8, stride=COLUMN), :]
                fill(read, code, guess, inverse, v, x, slice(y, y + 8), z)
        return carry

    lax.fori_loop(0, xs, step, 0)


def fields(tot, code):
    xs, _, nz = code.shape
    one = jax.ShapeDtypeStruct((xs, ROWS, nz), F32)
    three = jax.ShapeDtypeStruct((3, xs, ROWS, nz), F32)
    return call(fields_kernel, [vmem()] * 2, [vmem()] * 3, [three, one, three])(tot, code)


def edge_kernel(after, prior, code, guess_in, inverse_in, v_in, guess, inverse, v, to_next, to_prior, edge):
    xs, ys, zs = code.shape[0], ROWS - 8, code.shape[2] // LANES
    for x in range(xs):
        edge[pl.ds(x * 256, 96), :] = after[pl.ds(x * 96, 96), :]
        edge[pl.ds(x * 256 + 96, 64), :] = jnp.zeros((64, LANES), F32)
        edge[pl.ds(x * 256 + 160, 96), :] = prior[pl.ds(x * 96, 96), :]

    def step(x, carry):
        for z in range(zs):
            read = lambda c: edge[pl.ds(x * 256 + z * 4 + c, 8, stride=32), :]
            fill(read, code, guess, inverse, v, x, slice(ys, ROWS), z)
        return carry

    lax.fori_loop(0, xs, step, 0)
    send_layers(v, to_next, to_prior, xs, zs)


def add_edge(after, prior, code, guess, inverse, v):
    xs, _, nz = code.shape
    layer = jax.ShapeDtypeStruct((ROWS, nz), F32)
    shapes = [jax.ShapeDtypeStruct(a.shape, F32) for a in (guess, inverse, v)]
    return call(
        edge_kernel,
        [vmem()] * 6,
        [vmem()] * 5,
        shapes + [layer, layer],
        [pltpu.VMEM((xs * 256, LANES), F32)],
        limit=4,
        micros=1,
        input_output_aliases={3: 0, 4: 1, 5: 2},
    )(after, prior, code, guess, inverse, v)


def ascend(p_out, p_in, v, code, x, before, first, zs):
    spread = partial_spread(v, x, zs)
    for z in range(zs):
        s = spread[z] - before(z)
        old = -STEP * s if first else p_in[x, :, strip(z)] - STEP * s
        liquid = code[x, :, strip(z)] & LIQUID != 0
        p_out[x, :, strip(z)] = jnp.where(liquid, jnp.maximum(old, 0.0), 0.0)


def push(v_out, p, code, guess, inverse, x, after, zs):
    here = strips_of(p, (x,), zs)
    here_z = after_z(here)
    for z in range(zs):
        r = inverse[x, :, strip(z)]
        bits = code[x, :, strip(z)]
        beyond = (after(z), after_y(here[z]), here_z[z])
        for a in range(3):
            moved = guess[a, x, :, strip(z)] + (here[z] - beyond[a]) * r
            v_out[a, x, :, strip(z)] = jnp.where(bits & (1 << a) != 0, moved, 0.0)


def climb_inside(first, p_in, v_in, code, guess, inverse, p, v):
    xs, zs = code.shape[0], code.shape[2] // LANES

    def up(x, carry):
        ascend(p, p_in, v_in, code, x, lambda z: v_in[0, x - 1, :, strip(z)], first, zs)
        return carry

    lax.fori_loop(1, xs, up, 0)

    def out(x, carry):
        push(v, p, code, guess, inverse, x, lambda z: p[x + 1, :, strip(z)], zs)
        return carry

    lax.fori_loop(1, xs - 1, out, 0)


def climb_outside(first, before, spread, beyond, p8_in, p_in, v_in, code, guess, inverse, p, v, p8):
    xs, zs = code.shape[0], code.shape[2] // LANES
    ascend(p, p_in, v_in, code, 0, lambda z: before[:, strip(z)], first, zs)
    for z in range(zs):
        s = spread[:, strip(z)] - v_in[0, xs - 1, :, strip(z)]
        old = -STEP * s if first else p8_in[:, strip(z)] - STEP * s
        p8[:, strip(z)] = jnp.where(beyond[:, strip(z)] == 2, jnp.maximum(old, 0.0), 0.0)
    push(v, p, code, guess, inverse, 0, lambda z: p[1, :, strip(z)], zs)
    push(v, p, code, guess, inverse, xs - 1, lambda z: p8[:, strip(z)], zs)


def turn(v, guess, change, x):
    ys, zs = ROWS - 8, v.shape[3] // LANES
    for a in range(3):
        for z in range(zs):
            for y in range(0, ys, 8):
                at = (a, x, slice(y, y + 8), strip(z))
                change[pl.ds((x * ys + y) * COLUMN + z * 4 + a, 8, stride=COLUMN), :] = v[at] - guess[at]


def inner_first_kernel(v_in, code, guess, inverse, p, v):
    climb_inside(True, None, v_in, code, guess, inverse, p, v)


def inner_kernel(p_in, v_in, code, guess, inverse, p, v):
    climb_inside(False, p_in, v_in, code, guess, inverse, p, v)


def layer_copies(p, v, p_out, v_out, x, sem):
    ys = ROWS - 8
    rows = pl.ds(0, ys)
    yield pltpu.make_async_copy(p.at[x, rows], p_out.at[x], sem)
    for a in range(3):
        yield pltpu.make_async_copy(v.at[a, x, rows], v_out.at[a, x], sem)


def inner_last_kernel(p_in, v_in, code, guess, inverse, p, v, change, p_out, v_out, sem):
    climb_inside(False, p_in, v_in, code, guess, inverse, p, v)
    xs = code.shape[0]

    def step(x, carry):
        for copy in layer_copies(p, v, p_out, v_out, x, sem.at[x]):
            copy.start()
        turn(v, guess, change, x)
        return carry

    lax.fori_loop(1, xs - 1, step, 0)
    for x in range(1, xs - 1):
        for copy in layer_copies(p, v, p_out, v_out, x, sem.at[x]):
            copy.wait()


def outer_first_kernel(before, spread, beyond, p_in, v_in, code, guess, inverse, p, v, p8, to_next, to_prior):
    climb_outside(True, before, spread, beyond, None, p_in, v_in, code, guess, inverse, p, v, p8)
    send_layers(v, to_next, to_prior, code.shape[0], code.shape[2] // LANES)


def outer_kernel(before, spread, beyond, p8_in, p_in, v_in, code, guess, inverse, p, v, p8, to_next, to_prior):
    climb_outside(False, before, spread, beyond, p8_in, p_in, v_in, code, guess, inverse, p, v, p8)
    send_layers(v, to_next, to_prior, code.shape[0], code.shape[2] // LANES)


def outer_last_kernel(
    before, spread, beyond, p8_in, names, change_in, p_in, v_in, code, guess, inverse, p_out_in, v_out_in,
    p, v, change, p_out, v_out, reply_out, p8, reply, sem, reply_sem
):
    climb_outside(False, before, spread, beyond, p8_in, p_in, v_in, code, guess, inverse, p, v, p8)
    ends = (0, code.shape[0] - 1)
    for i, x in enumerate(ends):
        for copy in layer_copies(p, v, p_out, v_out, x, sem.at[i]):
            copy.start()
    for x in ends:
        turn(v, guess, change, x)
    steps = reply.shape[0] // 192

    def piece(g):
        rows = pl.ds(pl.multiple_of(g * 192, 192), 192)
        return pltpu.make_async_copy(reply.at[rows], reply_out.at[rows], reply_sem.at[g])

    def step(g, carry):
        base = pl.multiple_of(g * 192, 192)
        for k in range(64):
            b = names[g * 64 + k]
            reply[pl.ds(base + 3 * k, 3), :] = change[pl.ds((b >> 3) * COLUMN + (b & 7) * 4, 3), :]
        piece(g).start()
        return carry

    lax.fori_loop(0, steps, step, 0)

    def finish(g, carry):
        piece(g).wait()
        return carry

    lax.fori_loop(0, steps, finish, 0)
    for i, x in enumerate(ends):
        for copy in layer_copies(p, v, p_out, v_out, x, sem.at[i]):
            copy.wait()


def like(*arrays):
    return [jax.ShapeDtypeStruct(a.shape, F32) for a in arrays]


def climb(names, v, code, guess, inverse, beyond, to_next, to_prior):
    xs, _, nz = code.shape
    rows = xs * (ROWS - 8) * COLUMN + 8
    for sweep in range(ITERS):
        before = shifted(to_next, "slab", 1)
        spread = shifted(to_prior, "slab", -1)
        rest = (code, guess, inverse)
        if sweep == 0:
            p, v = call(
                inner_first_kernel, [vmem()] * 4, [vmem()] * 2, like(inverse, v), input_output_aliases={0: 1}
            )(v, *rest)
            p, v, p8, to_next, to_prior = call(
                outer_first_kernel,
                [vmem()] * 8,
                [vmem()] * 5,
                like(p, v, before, before, before),
                micros=1,
                input_output_aliases={3: 0, 4: 1},
            )(before, spread, beyond, p, v, *rest)
        elif sweep < ITERS - 1:
            p, v = call(
                inner_kernel, [vmem()] * 5, [vmem()] * 2, like(p, v), input_output_aliases={0: 0, 1: 1}
            )(p, v, *rest)
            p, v, p8, to_next, to_prior = call(
                outer_kernel,
                [vmem()] * 9,
                [vmem()] * 5,
                like(p, v, before, before, before),
                micros=1,
                input_output_aliases={4: 0, 5: 1},
            )(before, spread, beyond, p8, p, v, *rest)
        else:
            change = jax.ShapeDtypeStruct((rows, LANES), F32)
            p_out = jax.ShapeDtypeStruct((xs, ROWS - 8, nz), F32)
            v_out = jax.ShapeDtypeStruct((3, xs, ROWS - 8, nz), F32)
            p, v, change, p_out, v_out = call(
                inner_last_kernel,
                [vmem()] * 5,
                [vmem()] * 3 + [hbm()] * 2,
                like(p, v) + [change, p_out, v_out],
                [pltpu.SemaphoreType.DMA((xs,))],
                micros=5,
                input_output_aliases={0: 0, 1: 1},
            )(p, v, *rest)
            reply = jax.ShapeDtypeStruct((names.shape[0] * 3, LANES), F32)
            p, v, change, p_out, v_out, reply = call(
                outer_last_kernel,
                [vmem()] * 4 + [smem()] + [vmem()] * 6 + [hbm()] * 2,
                [vmem()] * 3 + [hbm()] * 3,
                like(p, v, change, p_out, v_out) + [reply],
                [
                    pltpu.VMEM(before.shape, F32),
                    pltpu.VMEM(reply.shape, F32),
                    pltpu.SemaphoreType.DMA((2,)),
                    pltpu.SemaphoreType.DMA((reply.shape[0] // 192,)),
                ],
                input_output_aliases={5: 2, 6: 0, 7: 1, 11: 3, 12: 4},
            )(before, spread, beyond, p8, names, change, p, v, *rest, p_out, v_out)
    return p_out, v_out, reply


def shifted(block, axis, distance):
    devices = range(lax.axis_size(axis))
    return lax.ppermute(block, axis, [(i - distance, i) for i in devices if i - distance in devices])


ITERS = 3


def on_device(velocity, weight, offset, owner, brick, flags):
    devices = lax.axis_size("slab") * lax.axis_size("sub")
    xs, ys, nz = flags.shape
    both = ("slab", "sub")
    kinds = jnp.where(flags == 2, 0, flags + 1)
    later = shifted(kinds[:, :4], "sub", -1)
    prior = shifted(kinds[:, ys - 3 :], "sub", 1)
    tile = jnp.concatenate([later, jnp.zeros((xs, 1, nz), I32), prior], 1)
    beyond = shifted(jnp.concatenate([kinds[0], tile[0]], 0), "slab", -1)
    planes = velocity.transpose(1, 0, 2)
    outgoing, place = splat(planes, weight, offset, owner[:, 0], brick[:, 0], devices)
    arrived = lax.all_to_all(outgoing.reshape(devices, 1, CHUNK * LANES), both, 0, 0, tiled=True)
    code = make_code(flags, tile, beyond)
    arrived, code, beyond = lax.optimization_barrier((arrived, code, beyond))
    names = arrived[:, 0, 32 * LANES : 32 * LANES + 8].astype(I32).reshape(-1)
    totals, first_rows, last_rows = scatter(arrived.reshape(devices * CHUNK, LANES), names, xs, ys)
    after = shifted(first_rows, "sub", -1)
    before = shifted(last_rows, "sub", 1)
    guess, inverse, v = fields(totals, code)
    guess, inverse, v, to_next, to_prior = add_edge(after, before, code, guess, inverse, v)
    p, v, reply = climb(names, v, code, guess, inverse, beyond, to_next, to_prior)
    back = lax.all_to_all(reply.reshape(devices, 24, LANES), both, 0, 0, tiled=True)
    updated = pick(back.reshape(devices * 24, LANES), planes, offset, place)
    return updated.transpose(1, 0, 2), p, v


def solution(mesh):
    return jax.shard_map(
        on_device,
        mesh=mesh,
        in_specs=(P(("slab", "sub")),) * 5 + (P("slab", "sub"),),
        out_specs=(P(("slab", "sub")), P("slab", "sub"), P(None, "slab", "sub")),
        check_vma=False,
    )
```

```python
import jax
import jax.numpy as jnp
from jax import lax
from jax.experimental import pallas as pl
from jax.experimental.pallas import tpu as pltpu
from jax.sharding import PartitionSpec as P


F32 = jnp.float32
BF16 = jnp.bfloat16
I32 = jnp.int32
LANES = 128
CHUNK = 33
COLUMN = 33
MIB = 1 << 20
GROUP = 128


def vmem():
    return pl.BlockSpec(memory_space=pltpu.VMEM)


def hbm():
    return pl.BlockSpec(memory_space=pltpu.HBM)


def smem():
    return pl.BlockSpec(memory_space=pltpu.SMEM)


def call(kernel, ins, outs, shapes, scratch=(), limit=3, micros=3, **kw):
    return pl.pallas_call(
        kernel,
        in_specs=ins,
        out_specs=outs,
        out_shape=shapes,
        scratch_shapes=list(scratch),
        compiler_params=pltpu.CompilerParams(vmem_limit_bytes=limit * MIB),
        cost_estimate=pl.CostEstimate(flops=micros * 100_000_000, bytes_accessed=1 << 20, transcendentals=0),
        **kw,
    )


def two_parts(x):
    high = x.astype(BF16).astype(F32)
    return high, x - high


def one_hot(offsets, cells):
    return jnp.where(jnp.broadcast_to(offsets, cells.shape) == cells, 1.0, 0.0).astype(BF16)


def splat_kernel(
    vel_hbm, weight_hbm, offset_hbm, owner_hbm, brick_hbm, out, place,
    vel, weight, offset, owner, brick, parts, names, count, sems
):
    pairs = ((vel_hbm, vel), (weight_hbm, weight), (offset_hbm, offset), (owner_hbm, owner), (brick_hbm, brick))
    copies = [pltpu.make_async_copy(a, b, sems.at[i]) for i, (a, b) in enumerate(pairs)]
    for copy in copies:
        copy.start()
    blocks = weight.shape[0]
    devices = names.shape[0]
    names[...] = jnp.full(names.shape, 4096.0, F32)

    def clear(g, carry):
        out[pl.ds(pl.multiple_of(g * 8, 8), 8), :] = jnp.zeros((8, LANES), F32)
        return carry

    lax.fori_loop(0, out.shape[0] // 8, clear, 0, unroll=16)

    def reset(d, carry):
        count[d] = 0
        return carry

    lax.fori_loop(0, devices, reset, 0, unroll=8)
    for copy in copies:
        copy.wait()

    def load(g, carry):
        for half in range(2):
            rows = pl.ds(pl.multiple_of(g * 16 + 8 * half, 8), 8)
            w = weight[rows, :]
            base = pl.multiple_of(g * 128, 128) + 4 * half
            for c in range(4):
                high, low = two_parts(vel[c, rows, :] * w if c < 3 else w)
                parts[pl.ds(base + c, 8, stride=16), :] = high
                parts[pl.ds(base + 8 + c, 8, stride=16), :] = low
        return carry

    lax.fori_loop(0, blocks // 16, load, 0, unroll=2)
    cells = lax.broadcasted_iota(I32, (LANES, LANES), 0)
    lane = lax.broadcasted_iota(I32, (1, LANES), 1)
    upper = lax.broadcasted_iota(I32, (16, LANES), 0) % 8 < 4

    def step(g, carry):
        base = pl.multiple_of(g * GROUP, GROUP)
        offs = offset[pl.ds(base, GROUP), :]
        sums = [None] * GROUP
        for t in range(GROUP // 16):
            for q in range(8):
                one, two = t * 16 + q, t * 16 + 8 + q
                hot = jnp.concatenate(
                    [one_hot(offs[one : one + 1, :], cells), one_hot(offs[two : two + 1, :], cells)], 1
                )
                x = parts[pl.ds(pl.multiple_of(base * 8, 8 * GROUP) + 128 * t + 16 * q, 16), :]
                lhs = jnp.concatenate([jnp.where(upper, x, 0.0), jnp.where(upper, 0.0, x)], 1).astype(BF16)
                r = lax.dot_general(lhs, hot, (((1,), (1,)), ((), ())), preferred_element_type=F32)
                r = r[0:8] + r[8:16]
                sums[one], sums[two] = r[0:4], r[4:8]
        for j in range(GROUP):
            d = owner[base + j]
            slot = count[d]
            count[d] = slot + 1
            place[base + j] = d * 8 + slot
            out[pl.ds(d * CHUNK + slot * 4, 4), :] = sums[j]
            b = brick[base + j]
            old = names[pl.ds(d, 1), :]
            names[pl.ds(d, 1), :] = jnp.where(lane == slot, jnp.full((1, LANES), b, I32).astype(F32), old)
        return carry

    lax.fori_loop(0, blocks // GROUP, step, 0)
    out[pl.ds(32, devices, stride=CHUNK), :] = names[...]


def splat(vel, weight, offset, owner, brick, devices):
    blocks = weight.shape[0]
    return call(
        splat_kernel,
        [hbm()] * 5,
        [vmem(), smem()],
        [jax.ShapeDtypeStruct((devices * CHUNK, LANES), F32), jax.ShapeDtypeStruct((blocks,), I32)],
        [
            pltpu.VMEM(vel.shape, F32),
            pltpu.VMEM(weight.shape, F32),
            pltpu.VMEM(offset.shape, I32),
            pltpu.SMEM((blocks,), I32),
            pltpu.SMEM((blocks,), I32),
            pltpu.VMEM((blocks * 8, LANES), F32),
            pltpu.VMEM((devices, LANES), F32),
            pltpu.SMEM((devices,), I32),
            pltpu.SemaphoreType.DMA((5,)),
        ],
        limit=60,
        micros=8,
    )(vel, weight, offset, owner, brick)


def pick_kernel(ret, vel, offset, place, out, parts, sums):
    blocks = offset.shape[0]
    cells = lax.broadcasted_iota(I32, (LANES, LANES), 0)
    upper = lax.broadcasted_iota(I32, (8, LANES), 0) < 4

    def gather(g, carry):
        base = pl.multiple_of(g * 16, 16)
        for j in range(16):
            high, low = two_parts(ret[pl.ds(place[base + j] * 3, 3), :])
            at = pl.multiple_of(base * 8, 128) + 16 * (j % 8) + 4 * (j // 8)
            parts[pl.ds(at, 3), :] = high
            parts[pl.ds(at + 8, 3), :] = low
        return carry

    lax.fori_loop(0, blocks // 16, gather, 0)

    def step(g, carry):
        base = pl.multiple_of(g * GROUP, GROUP)
        offs = offset[pl.ds(base, GROUP), :]
        for t in range(GROUP // 16):
            for q in range(8):
                one, two = t * 16 + q, t * 16 + 8 + q
                hot = jnp.concatenate(
                    [one_hot(offs[one : one + 1, :], cells), one_hot(offs[two : two + 1, :], cells)], 1
                )
                lhs = parts[pl.ds(pl.multiple_of(base * 8, 8 * GROUP) + 128 * t + 16 * q, 16), :].astype(BF16)
                r = lax.dot_general(lhs, hot, (((1,), (0,)), ((), ())), preferred_element_type=F32)
                r = r[0:8] + r[8:16]
                at = pl.multiple_of(base * 4, 4 * GROUP) + 64 * t + 8 * q
                sums[pl.ds(at, 8), :] = jnp.where(upper, r[:, :LANES], r[:, LANES:])
        return carry

    lax.fori_loop(0, blocks // GROUP, step, 0)

    def add(g, carry):
        for half in range(2):
            rows = pl.ds(pl.multiple_of(g * 16 + 8 * half, 8), 8)
            for c in range(3):
                change = sums[pl.ds(pl.multiple_of(g * 64, 64) + 4 * half + c, 8, stride=8), :]
                out[c, rows, :] = vel[c, rows, :] + change
        return carry

    lax.fori_loop(0, blocks // 16, add, 0, unroll=4)


def pick(ret, vel, offset, place):
    blocks = offset.shape[0]
    return call(
        pick_kernel,
        [vmem()] * 3 + [smem()],
        vmem(),
        jax.ShapeDtypeStruct((3, blocks, LANES), F32),
        [pltpu.VMEM((blocks * 8, LANES), F32), pltpu.VMEM((blocks * 4, LANES), F32)],
        limit=12,
        micros=6,
    )(ret, vel, offset, place)


def scatter_kernel(arr_hbm, names, tot, first, last, arr, sem):
    xs, ys = first.shape[0] // 96, 64
    per = 8 * CHUNK
    load = pltpu.make_async_copy(arr_hbm, arr, sem.at[0])
    load.start()

    def clear(g, carry):
        tot[pl.ds(pl.multiple_of(g * 8, 8), 8), :] = jnp.zeros((8, LANES), F32)
        return carry

    lax.fori_loop(0, tot.shape[0] // 8, clear, 0, unroll=16)
    load.wait()

    def step(g, carry):
        base = pl.multiple_of(g * per, 8)
        for first_slot in range(0, 64, 4):
            slots = range(first_slot, first_slot + 4)
            rows = []
            for k in slots:
                b = names[g * 64 + k]
                rows.append((b >> 3) * COLUMN + (b & 7) * 4)
            old = [tot[pl.ds(row, 4), :] for row in rows]
            new = [arr[pl.ds(base + (k // 8) * CHUNK + (k % 8) * 4, 4), :] for k in slots]
            for i in range(4):
                total = old[i] + new[i]
                for j in range(i):
                    total = total + jnp.where(rows[j] == rows[i], new[j], 0.0)
                tot[pl.ds(rows[i], 4), :] = total
        return carry

    lax.fori_loop(0, arr.shape[0] // per, step, 0)
    for x in range(xs):
        for r in range(3):
            first[pl.ds(x * 96 + r * 32, 32), :] = tot[pl.ds((x * ys + r) * COLUMN, 32), :]
            last[pl.ds(x * 96 + r * 32, 32), :] = tot[pl.ds((x * ys + ys - 3 + r) * COLUMN, 32), :]


def scatter(arr, names, xs, ys):
    rows = xs * ys * COLUMN + 8
    halo = jax.ShapeDtypeStruct((xs * 96, LANES), F32)
    return call(
        scatter_kernel,
        [hbm(), smem()],
        [vmem()] * 3,
        [jax.ShapeDtypeStruct((rows, LANES), F32), halo, halo],
        [pltpu.VMEM(arr.shape, F32), pltpu.SemaphoreType.DMA((1,))],
    )(arr, names)


ROWS = 72
LIQUID = 8
STEP = 0.15


def strip(z):
    return pl.ds(z * LANES, LANES)


def lanes():
    return lax.broadcasted_iota(I32, (ROWS, LANES), 1)


def before_y(a):
    return pltpu.roll(a, 1, 0)


def after_y(a):
    return pltpu.roll(a, ROWS - 1, 0)


def before_z(strips):
    lane = lanes()
    rolled = [pltpu.roll(a, 1, 1) for a in strips]
    return [jnp.where(lane == 0, rolled[z - 1], rolled[z]) for z in range(len(strips))]


def after_z(strips):
    lane = lanes()
    rolled = [pltpu.roll(a, LANES - 1, 1) for a in strips]
    last = len(strips) - 1
    return [jnp.where(lane == LANES - 1, rolled[z + 1 if z < last else 0], rolled[z]) for z in range(len(strips))]


def strips_of(ref, index, count):
    return [ref[(*index, slice(None), strip(z))] for z in range(count)]


def kind(f):
    return jnp.where(f == 2, 0, f + 1)


def ends_kernel(flags, layer_out, low_out, high_out, layer, low, high, sems):
    ys = flags.shape[1]
    copies = [
        pltpu.make_async_copy(flags.at[0], layer, sems.at[0]),
        pltpu.make_async_copy(flags.at[:, pl.ds(0, 8)], low, sems.at[1]),
        pltpu.make_async_copy(flags.at[:, pl.ds(ys - 8, 8)], high, sems.at[2]),
    ]
    for copy in copies:
        copy.start()
    for copy in copies:
        copy.wait()
    layer_out[...] = kind(layer[...])
    low_out[...] = kind(low[...])[:, :4]
    high_out[...] = kind(high[...])[:, 4:]


def flag_ends(flags):
    xs, ys, nz = flags.shape
    layer, rows, few = ((ys, nz), (xs, 8, nz), (xs, 4, nz))
    return call(
        ends_kernel,
        [hbm()],
        [vmem()] * 3,
        [jax.ShapeDtypeStruct(a, I32) for a in (layer, few, few)],
        [pltpu.VMEM(a, I32) for a in (layer, rows, rows)] + [pltpu.SemaphoreType.DMA((3,))],
        limit=62,
        micros=1,
    )(flags)


def code_kernel(flags, tile, beyond, code):
    xs, zs = code.shape[0], code.shape[2] // LANES

    def encoded(x):
        def one(z):
            return jnp.concatenate([kind(flags[x, :, strip(z)]), tile[x, :, strip(z)]], 0)

        return [one(z) for z in range(zs)]

    def layer(x, e, e_next):
        o = [jnp.minimum(a, 1) for a in e]
        o_z = after_z(o)
        lane = lanes()
        o_z[-1] = jnp.where(lane == LANES - 1, 0, o_z[-1])
        for z in range(zs):
            c = o[z] & jnp.minimum(e_next[z], 1)
            c = c | ((o[z] & after_y(o[z])) << 1) | ((o[z] & o_z[z]) << 2)
            code[x, :, strip(z)] = c | jnp.where(e[z] == 2, LIQUID, 0)

    def step(x, carry):
        layer(x, encoded(x), encoded(x + 1))
        return carry

    lax.fori_loop(0, xs - 1, step, 0)
    layer(xs - 1, encoded(xs - 1), strips_of(beyond, (), zs))


def make_code(flags, tile, beyond):
    xs, _, nz = flags.shape
    return call(
        code_kernel, [vmem()] * 3, vmem(), jax.ShapeDtypeStruct((xs, ROWS, nz), I32)
    )(flags, tile, beyond)


def partial_spread(v, x, zs):
    vx, vy, vz = (strips_of(v, (a, x), zs) for a in range(3))
    vz_before = before_z(vz)
    return [vx[z] + (vy[z] - before_y(vy[z])) + (vz[z] - vz_before[z]) for z in range(zs)]


def send_layers(v, to_next, to_prior, xs, zs):
    for z, s in enumerate(partial_spread(v, 0, zs)):
        to_prior[:, strip(z)] = s
    to_next[...] = v[0, xs - 1]


def fill(read, code, guess, inverse, v, x, rows, z):
    at = (x, rows, strip(z))
    r = 1.0 / (read(3) + 1.0)
    inverse[at] = r
    bits = code[at]
    for a in range(3):
        g = read(a) * r
        guess[(a, *at)] = g
        v[(a, *at)] = jnp.where(bits & (1 << a) != 0, g, 0.0)


def fields_kernel(tot, code, guess, inverse, v):
    xs, ys, zs = code.shape[0], ROWS - 8, code.shape[2] // LANES

    def step(x, carry):
        for z in range(zs):
            for y in range(0, ys, 8):
                start = (x * ys + y) * COLUMN + z * 4
                read = lambda c: tot[pl.ds(start + c, 8, stride=COLUMN), :]
                fill(read, code, guess, inverse, v, x, slice(y, y + 8), z)
        return carry

    lax.fori_loop(0, xs, step, 0)


def fields(tot, code):
    xs, _, nz = code.shape
    one = jax.ShapeDtypeStruct((xs, ROWS, nz), F32)
    three = jax.ShapeDtypeStruct((3, xs, ROWS, nz), F32)
    return call(fields_kernel, [vmem()] * 2, [vmem()] * 3, [three, one, three])(tot, code)


def edge_kernel(after, prior, code, guess_in, inverse_in, v_in, guess, inverse, v, to_next, to_prior, edge):
    xs, ys, zs = code.shape[0], ROWS - 8, code.shape[2] // LANES
    for x in range(xs):
        edge[pl.ds(x * 256, 96), :] = after[pl.ds(x * 96, 96), :]
        edge[pl.ds(x * 256 + 96, 64), :] = jnp.zeros((64, LANES), F32)
        edge[pl.ds(x * 256 + 160, 96), :] = prior[pl.ds(x * 96, 96), :]

    def step(x, carry):
        for z in range(zs):
            read = lambda c: edge[pl.ds(x * 256 + z * 4 + c, 8, stride=32), :]
            fill(read, code, guess, inverse, v, x, slice(ys, ROWS), z)
        return carry

    lax.fori_loop(0, xs, step, 0)
    send_layers(v, to_next, to_prior, xs, zs)


def add_edge(after, prior, code, guess, inverse, v):
    xs, _, nz = code.shape
    layer = jax.ShapeDtypeStruct((ROWS, nz), F32)
    shapes = [jax.ShapeDtypeStruct(a.shape, F32) for a in (guess, inverse, v)]
    return call(
        edge_kernel,
        [vmem()] * 6,
        [vmem()] * 5,
        shapes + [layer, layer],
        [pltpu.VMEM((xs * 256, LANES), F32)],
        limit=4,
        micros=1,
        input_output_aliases={3: 0, 4: 1, 5: 2},
    )(after, prior, code, guess, inverse, v)


def ascend(p_out, p_in, v, code, x, before, first, zs):
    spread = partial_spread(v, x, zs)
    for z in range(zs):
        s = spread[z] - before(z)
        old = -STEP * s if first else p_in[x, :, strip(z)] - STEP * s
        liquid = code[x, :, strip(z)] & LIQUID != 0
        p_out[x, :, strip(z)] = jnp.where(liquid, jnp.maximum(old, 0.0), 0.0)


def push(v_out, p, code, guess, inverse, x, after, zs, axes=(0, 1, 2)):
    here = strips_of(p, (x,), zs)
    here_z = after_z(here) if 2 in axes else here
    for z in range(zs):
        r = inverse[x, :, strip(z)]
        bits = code[x, :, strip(z)]
        beyond = (after(z) if 0 in axes else None, after_y(here[z]), here_z[z])
        for a in axes:
            moved = guess[a, x, :, strip(z)] + (here[z] - beyond[a]) * r
            v_out[a, x, :, strip(z)] = jnp.where(bits & (1 << a) != 0, moved, 0.0)


def climb_inside(first, p_in, v_in, code, guess, inverse, p, v):
    xs, zs = code.shape[0], code.shape[2] // LANES

    def up(x, carry):
        ascend(p, p_in, v_in, code, x, lambda z: v_in[0, x - 1, :, strip(z)], first, zs)
        return carry

    lax.fori_loop(1, xs, up, 0)

    def out(x, carry):
        push(v, p, code, guess, inverse, x, lambda z: p[x + 1, :, strip(z)], zs)
        return carry

    lax.fori_loop(1, xs - 1, out, 0)
    push(v, p, code, guess, inverse, xs - 1, None, zs, (1, 2))


def climb_outside(first, before, spread, beyond, p8_in, p_in, v_in, code, guess, inverse, p, v, p8):
    xs, zs = code.shape[0], code.shape[2] // LANES
    ascend(p, p_in, v_in, code, 0, lambda z: before[:, strip(z)], first, zs)
    for z in range(zs):
        s = spread[:, strip(z)] - v_in[0, xs - 1, :, strip(z)]
        old = -STEP * s if first else p8_in[:, strip(z)] - STEP * s
        p8[:, strip(z)] = jnp.where(beyond[:, strip(z)] == 2, jnp.maximum(old, 0.0), 0.0)
    push(v, p, code, guess, inverse, 0, lambda z: p[1, :, strip(z)], zs)
    push(v, p, code, guess, inverse, xs - 1, lambda z: p8[:, strip(z)], zs, (0,))


def turn(v, guess, change, x, axes=(0, 1, 2)):
    ys, zs = ROWS - 8, v.shape[3] // LANES
    for a in axes:
        for z in range(zs):
            for y in range(0, ys, 8):
                at = (a, x, slice(y, y + 8), strip(z))
                change[pl.ds((x * ys + y) * COLUMN + z * 4 + a, 8, stride=COLUMN), :] = v[at] - guess[at]


def inner_first_kernel(v_in, code, guess, inverse, p, v):
    climb_inside(True, None, v_in, code, guess, inverse, p, v)


def inner_kernel(p_in, v_in, code, guess, inverse, p, v):
    climb_inside(False, p_in, v_in, code, guess, inverse, p, v)


def copy_pressure(p, p_out, x, sem):
    return pltpu.make_async_copy(p.at[x, pl.ds(0, ROWS - 8)], p_out.at[x], sem)


def copy_faces(v, v_out, a, x, sem):
    return pltpu.make_async_copy(v.at[a, x, pl.ds(0, ROWS - 8)], v_out.at[a, x], sem)


def inner_last_kernel(p_in, v_in, code, guess, inverse, p, v, change, p_out, v_out, sem):
    climb_inside(False, p_in, v_in, code, guess, inverse, p, v)
    xs = code.shape[0]

    def copies(x, axes):
        return [copy_pressure(p, p_out, x, sem.at[x])] + [copy_faces(v, v_out, a, x, sem.at[x]) for a in axes]

    for copy in copies(xs - 1, (1, 2)):
        copy.start()

    def step(x, carry):
        for copy in copies(x, (0, 1, 2)):
            copy.start()
        turn(v, guess, change, x)
        return carry

    lax.fori_loop(1, xs - 1, step, 0)
    turn(v, guess, change, xs - 1, (1, 2))
    for x in range(1, xs):
        for copy in copies(x, (0, 1, 2) if x < xs - 1 else (1, 2)):
            copy.wait()


def outer_first_kernel(before, spread, beyond, p_in, v_in, code, guess, inverse, p, v, p8, to_next, to_prior):
    climb_outside(True, before, spread, beyond, None, p_in, v_in, code, guess, inverse, p, v, p8)
    send_layers(v, to_next, to_prior, code.shape[0], code.shape[2] // LANES)


def outer_kernel(before, spread, beyond, p8_in, p_in, v_in, code, guess, inverse, p, v, p8, to_next, to_prior):
    climb_outside(False, before, spread, beyond, p8_in, p_in, v_in, code, guess, inverse, p, v, p8)
    send_layers(v, to_next, to_prior, code.shape[0], code.shape[2] // LANES)


def outer_last_kernel(
    before, spread, beyond, p8_in, names, change_in, p_in, v_in, code, guess, inverse, p_out_in, v_out_in,
    p, v, change, p_out, v_out, reply, p8, sem
):
    climb_outside(False, before, spread, beyond, p8_in, p_in, v_in, code, guess, inverse, p, v, p8)
    end = code.shape[0] - 1
    copies = [copy_pressure(p, p_out, 0, sem.at[0])]
    copies += [copy_faces(v, v_out, a, 0, sem.at[0]) for a in range(3)]
    copies.append(copy_faces(v, v_out, 0, end, sem.at[0]))
    for copy in copies:
        copy.start()
    turn(v, guess, change, 0)
    turn(v, guess, change, end, (0,))

    def step(g, carry):
        base = pl.multiple_of(g * 192, 192)
        for k in range(64):
            b = names[g * 64 + k]
            reply[pl.ds(base + 3 * k, 3), :] = change[pl.ds((b >> 3) * COLUMN + (b & 7) * 4, 3), :]
        return carry

    lax.fori_loop(0, reply.shape[0] // 192, step, 0)
    for copy in copies:
        copy.wait()


def like(*arrays):
    return [jax.ShapeDtypeStruct(a.shape, F32) for a in arrays]


def climb(names, v, code, guess, inverse, beyond, to_next, to_prior):
    xs, _, nz = code.shape
    rows = xs * (ROWS - 8) * COLUMN + 8
    for sweep in range(ITERS):
        before = shifted(to_next, "slab", 1)
        spread = shifted(to_prior, "slab", -1)
        rest = (code, guess, inverse)
        if sweep == 0:
            p, v = call(
                inner_first_kernel, [vmem()] * 4, [vmem()] * 2, like(inverse, v), input_output_aliases={0: 1}
            )(v, *rest)
            p, v, p8, to_next, to_prior = call(
                outer_first_kernel,
                [vmem()] * 8,
                [vmem()] * 5,
                like(p, v, before, before, before),
                micros=1,
                input_output_aliases={3: 0, 4: 1},
            )(before, spread, beyond, p, v, *rest)
        elif sweep < ITERS - 1:
            p, v = call(
                inner_kernel, [vmem()] * 5, [vmem()] * 2, like(p, v), input_output_aliases={0: 0, 1: 1}
            )(p, v, *rest)
            p, v, p8, to_next, to_prior = call(
                outer_kernel,
                [vmem()] * 9,
                [vmem()] * 5,
                like(p, v, before, before, before),
                micros=1,
                input_output_aliases={4: 0, 5: 1},
            )(before, spread, beyond, p8, p, v, *rest)
        else:
            change = jax.ShapeDtypeStruct((rows, LANES), F32)
            p_out = jax.ShapeDtypeStruct((xs, ROWS - 8, nz), F32)
            v_out = jax.ShapeDtypeStruct((3, xs, ROWS - 8, nz), F32)
            p, v, change, p_out, v_out = call(
                inner_last_kernel,
                [vmem()] * 5,
                [vmem()] * 3 + [hbm()] * 2,
                like(p, v) + [change, p_out, v_out],
                [pltpu.SemaphoreType.DMA((xs,))],
                micros=5,
                input_output_aliases={0: 0, 1: 1},
            )(p, v, *rest)
            reply = jax.ShapeDtypeStruct((names.shape[0] * 3, LANES), F32)
            p, v, change, p_out, v_out, reply = call(
                outer_last_kernel,
                [vmem()] * 4 + [smem()] + [vmem()] * 6 + [hbm()] * 2,
                [vmem()] * 3 + [hbm()] * 2 + [vmem()],
                like(p, v, change, p_out, v_out) + [reply],
                [
                    pltpu.VMEM(before.shape, F32),
                    pltpu.SemaphoreType.DMA((1,)),
                ],
                input_output_aliases={5: 2, 6: 0, 7: 1, 11: 3, 12: 4},
            )(before, spread, beyond, p8, names, change, p, v, *rest, p_out, v_out)
    return p_out, v_out, reply


def shifted(block, axis, distance):
    devices = range(lax.axis_size(axis))
    return lax.ppermute(block, axis, [(i - distance, i) for i in devices if i - distance in devices])


ITERS = 3


def on_device(velocity, weight, offset, owner, brick, flags):
    devices = lax.axis_size("slab") * lax.axis_size("sub")
    xs, ys, _ = flags.shape
    both = ("slab", "sub")
    layer, low, high = flag_ends(flags)
    beyond_own = shifted(layer, "slab", -1)
    later = shifted(low, "sub", -1)
    prior = shifted(high, "sub", 1)
    planes = velocity.transpose(1, 0, 2)
    outgoing, place = splat(planes, weight, offset, owner[:, 0], brick[:, 0], devices)
    tile = jnp.concatenate([later, prior], 1)
    beyond = jnp.concatenate([beyond_own, shifted(tile[0], "slab", -1)], 0)
    arrived = lax.all_to_all(outgoing.reshape(devices, 1, CHUNK * LANES), both, 0, 0, tiled=True)
    code = make_code(flags, tile, beyond)
    arrived, code, beyond = lax.optimization_barrier((arrived, code, beyond))
    names = arrived[:, 0, 32 * LANES : 32 * LANES + 8].astype(I32).reshape(-1)
    totals, first_rows, last_rows = scatter(arrived.reshape(devices * CHUNK, LANES), names, xs, ys)
    after = shifted(first_rows, "sub", -1)
    before = shifted(last_rows, "sub", 1)
    guess, inverse, v = fields(totals, code)
    guess, inverse, v, to_next, to_prior = add_edge(after, before, code, guess, inverse, v)
    p, v, reply = climb(names, v, code, guess, inverse, beyond, to_next, to_prior)
    back = lax.all_to_all(reply.reshape(devices, 24, LANES), both, 0, 0, tiled=True)
    updated = pick(back.reshape(devices * 24, LANES), planes, offset, place)
    return updated.transpose(1, 0, 2), p, v


def solution(mesh):
    return jax.shard_map(
        on_device,
        mesh=mesh,
        in_specs=(P(("slab", "sub")),) * 5 + (P("slab", "sub"),),
        out_specs=(P(("slab", "sub")), P("slab", "sub"), P(None, "slab", "sub")),
        check_vma=False,
    )
```

```python
import jax
import jax.numpy as jnp
from jax import lax
from jax.experimental import pallas as pl
from jax.experimental.pallas import tpu as pltpu
from jax.sharding import PartitionSpec as P


F32 = jnp.float32
BF16 = jnp.bfloat16
I32 = jnp.int32
LANES = 128
CHUNK = 33
COLUMN = 33
MIB = 1 << 20
GROUP = 128


def vmem():
    return pl.BlockSpec(memory_space=pltpu.VMEM)


def hbm():
    return pl.BlockSpec(memory_space=pltpu.HBM)


def smem():
    return pl.BlockSpec(memory_space=pltpu.SMEM)


def call(kernel, ins, outs, shapes, scratch=(), limit=3, micros=3, **kw):
    return pl.pallas_call(
        kernel,
        in_specs=ins,
        out_specs=outs,
        out_shape=shapes,
        scratch_shapes=list(scratch),
        compiler_params=pltpu.CompilerParams(vmem_limit_bytes=limit * MIB),
        cost_estimate=pl.CostEstimate(flops=micros * 100_000_000, bytes_accessed=1 << 20, transcendentals=0),
        **kw,
    )


def two_parts(x):
    high = x.astype(BF16).astype(F32)
    return high, x - high


def one_hot(offsets, cells):
    return jnp.where(jnp.broadcast_to(offsets, cells.shape) == cells, 1.0, 0.0).astype(BF16)


def splat_kernel(
    vel_hbm, weight_hbm, offset_hbm, owner_hbm, brick_hbm, out, place,
    vel, weight, offset, owner, brick, parts, names, count, sems
):
    pairs = ((vel_hbm, vel), (weight_hbm, weight), (offset_hbm, offset), (owner_hbm, owner), (brick_hbm, brick))
    copies = [pltpu.make_async_copy(a, b, sems.at[i]) for i, (a, b) in enumerate(pairs)]
    for copy in copies:
        copy.start()
    blocks = weight.shape[0]
    devices = names.shape[0]
    names[...] = jnp.full(names.shape, 4096.0, F32)

    def clear(g, carry):
        out[pl.ds(pl.multiple_of(g * 8, 8), 8), :] = jnp.zeros((8, LANES), F32)
        return carry

    lax.fori_loop(0, out.shape[0] // 8, clear, 0, unroll=16)

    def reset(d, carry):
        count[d] = 0
        return carry

    lax.fori_loop(0, devices, reset, 0, unroll=8)
    for copy in copies:
        copy.wait()

    def load(g, carry):
        for half in range(2):
            rows = pl.ds(pl.multiple_of(g * 16 + 8 * half, 8), 8)
            w = weight[rows, :]
            base = pl.multiple_of(g * 128, 128) + 4 * half
            for c in range(4):
                high, low = two_parts(vel[c, rows, :] * w if c < 3 else w)
                parts[pl.ds(base + c, 8, stride=16), :] = high
                parts[pl.ds(base + 8 + c, 8, stride=16), :] = low
        return carry

    lax.fori_loop(0, blocks // 16, load, 0, unroll=2)
    cells = lax.broadcasted_iota(I32, (LANES, LANES), 0)
    lane = lax.broadcasted_iota(I32, (1, LANES), 1)
    upper = lax.broadcasted_iota(I32, (16, LANES), 0) % 8 < 4

    def step(g, carry):
        base = pl.multiple_of(g * GROUP, GROUP)
        offs = offset[pl.ds(base, GROUP), :]
        sums = [None] * GROUP
        for t in range(GROUP // 16):
            for q in range(8):
                one, two = t * 16 + q, t * 16 + 8 + q
                hot = jnp.concatenate(
                    [one_hot(offs[one : one + 1, :], cells), one_hot(offs[two : two + 1, :], cells)], 1
                )
                x = parts[pl.ds(pl.multiple_of(base * 8, 8 * GROUP) + 128 * t + 16 * q, 16), :]
                lhs = jnp.concatenate([jnp.where(upper, x, 0.0), jnp.where(upper, 0.0, x)], 1).astype(BF16)
                r = lax.dot_general(lhs, hot, (((1,), (1,)), ((), ())), preferred_element_type=F32)
                r = r[0:8] + r[8:16]
                sums[one], sums[two] = r[0:4], r[4:8]
        for j in range(GROUP):
            d = owner[base + j]
            slot = count[d]
            count[d] = slot + 1
            place[base + j] = d * 8 + slot
            out[pl.ds(d * CHUNK + slot * 4, 4), :] = sums[j]
            b = brick[base + j]
            old = names[pl.ds(d, 1), :]
            names[pl.ds(d, 1), :] = jnp.where(lane == slot, jnp.full((1, LANES), b, I32).astype(F32), old)
        return carry

    lax.fori_loop(0, blocks // GROUP, step, 0)
    out[pl.ds(32, devices, stride=CHUNK), :] = names[...]


def splat(vel, weight, offset, owner, brick, devices):
    blocks = weight.shape[0]
    return call(
        splat_kernel,
        [hbm()] * 5,
        [vmem(), smem()],
        [jax.ShapeDtypeStruct((devices * CHUNK, LANES), F32), jax.ShapeDtypeStruct((blocks,), I32)],
        [
            pltpu.VMEM(vel.shape, F32),
            pltpu.VMEM(weight.shape, F32),
            pltpu.VMEM(offset.shape, I32),
            pltpu.SMEM((blocks,), I32),
            pltpu.SMEM((blocks,), I32),
            pltpu.VMEM((blocks * 8, LANES), F32),
            pltpu.VMEM((devices, LANES), F32),
            pltpu.SMEM((devices,), I32),
            pltpu.SemaphoreType.DMA((5,)),
        ],
        limit=60,
        micros=8,
    )(vel, weight, offset, owner, brick)


def pick_kernel(ret, vel, offset, place, out, parts, sums):
    blocks = offset.shape[0]
    cells = lax.broadcasted_iota(I32, (LANES, LANES), 0)
    upper = lax.broadcasted_iota(I32, (8, LANES), 0) < 4

    def gather(g, carry):
        base = pl.multiple_of(g * 16, 16)
        for j in range(16):
            high, low = two_parts(ret[pl.ds(place[base + j] * 3, 3), :])
            at = pl.multiple_of(base * 8, 128) + 16 * (j % 8) + 4 * (j // 8)
            parts[pl.ds(at, 3), :] = high
            parts[pl.ds(at + 8, 3), :] = low
        return carry

    lax.fori_loop(0, blocks // 16, gather, 0)

    def step(g, carry):
        base = pl.multiple_of(g * GROUP, GROUP)
        offs = offset[pl.ds(base, GROUP), :]
        for t in range(GROUP // 16):
            for q in range(8):
                one, two = t * 16 + q, t * 16 + 8 + q
                hot = jnp.concatenate(
                    [one_hot(offs[one : one + 1, :], cells), one_hot(offs[two : two + 1, :], cells)], 1
                )
                lhs = parts[pl.ds(pl.multiple_of(base * 8, 8 * GROUP) + 128 * t + 16 * q, 16), :].astype(BF16)
                r = lax.dot_general(lhs, hot, (((1,), (0,)), ((), ())), preferred_element_type=F32)
                r = r[0:8] + r[8:16]
                at = pl.multiple_of(base * 4, 4 * GROUP) + 64 * t + 8 * q
                sums[pl.ds(at, 8), :] = jnp.where(upper, r[:, :LANES], r[:, LANES:])
        return carry

    lax.fori_loop(0, blocks // GROUP, step, 0)

    def add(g, carry):
        for half in range(2):
            rows = pl.ds(pl.multiple_of(g * 16 + 8 * half, 8), 8)
            for c in range(3):
                change = sums[pl.ds(pl.multiple_of(g * 64, 64) + 4 * half + c, 8, stride=8), :]
                out[c, rows, :] = vel[c, rows, :] + change
        return carry

    lax.fori_loop(0, blocks // 16, add, 0, unroll=4)


def pick(ret, vel, offset, place):
    blocks = offset.shape[0]
    return call(
        pick_kernel,
        [vmem()] * 3 + [smem()],
        vmem(),
        jax.ShapeDtypeStruct((3, blocks, LANES), F32),
        [pltpu.VMEM((blocks * 8, LANES), F32), pltpu.VMEM((blocks * 4, LANES), F32)],
        limit=12,
        micros=6,
    )(ret, vel, offset, place)


def scatter_kernel(arr_hbm, names, tot, first, last, arr, sem):
    xs, ys = first.shape[0] // 96, 64
    per = 8 * CHUNK
    load = pltpu.make_async_copy(arr_hbm, arr, sem.at[0])
    load.start()

    def clear(g, carry):
        tot[pl.ds(pl.multiple_of(g * 8, 8), 8), :] = jnp.zeros((8, LANES), F32)
        return carry

    lax.fori_loop(0, tot.shape[0] // 8, clear, 0, unroll=16)
    load.wait()

    def step(g, carry):
        base = pl.multiple_of(g * per, 8)
        for first_slot in range(0, 64, 4):
            slots = range(first_slot, first_slot + 4)
            rows = []
            for k in slots:
                b = names[g * 64 + k]
                rows.append((b >> 3) * COLUMN + (b & 7) * 4)
            old = [tot[pl.ds(row, 4), :] for row in rows]
            new = [arr[pl.ds(base + (k // 8) * CHUNK + (k % 8) * 4, 4), :] for k in slots]
            for i in range(4):
                total = old[i] + new[i]
                for j in range(i):
                    total = total + jnp.where(rows[j] == rows[i], new[j], 0.0)
                tot[pl.ds(rows[i], 4), :] = total
        return carry

    lax.fori_loop(0, arr.shape[0] // per, step, 0)
    for x in range(xs):
        for r in range(3):
            first[pl.ds(x * 96 + r * 32, 32), :] = tot[pl.ds((x * ys + r) * COLUMN, 32), :]
            last[pl.ds(x * 96 + r * 32, 32), :] = tot[pl.ds((x * ys + ys - 3 + r) * COLUMN, 32), :]


def scatter(arr, names, xs, ys):
    rows = xs * ys * COLUMN + 8
    halo = jax.ShapeDtypeStruct((xs * 96, LANES), F32)
    return call(
        scatter_kernel,
        [hbm(), smem()],
        [vmem()] * 3,
        [jax.ShapeDtypeStruct((rows, LANES), F32), halo, halo],
        [pltpu.VMEM(arr.shape, F32), pltpu.SemaphoreType.DMA((1,))],
    )(arr, names)


ROWS = 72
LIQUID = 8
STEP = 0.15


def strip(z):
    return pl.ds(z * LANES, LANES)


def lanes():
    return lax.broadcasted_iota(I32, (ROWS, LANES), 1)


def before_y(a):
    return pltpu.roll(a, 1, 0)


def after_y(a):
    return pltpu.roll(a, ROWS - 1, 0)


def before_z(strips):
    lane = lanes()
    rolled = [pltpu.roll(a, 1, 1) for a in strips]
    return [jnp.where(lane == 0, rolled[z - 1], rolled[z]) for z in range(len(strips))]


def after_z(strips):
    lane = lanes()
    rolled = [pltpu.roll(a, LANES - 1, 1) for a in strips]
    last = len(strips) - 1
    return [jnp.where(lane == LANES - 1, rolled[z + 1 if z < last else 0], rolled[z]) for z in range(len(strips))]


def strips_of(ref, index, count):
    return [ref[(*index, slice(None), strip(z))] for z in range(count)]


def kind(f):
    return jnp.where(f == 2, 0, f + 1)


def ends_kernel(flags, layer_out, low_out, high_out, layer, low, high, sems):
    ys = flags.shape[1]
    copies = [
        pltpu.make_async_copy(flags.at[0], layer, sems.at[0]),
        pltpu.make_async_copy(flags.at[:, pl.ds(0, 8)], low, sems.at[1]),
        pltpu.make_async_copy(flags.at[:, pl.ds(ys - 8, 8)], high, sems.at[2]),
    ]
    for copy in copies:
        copy.start()
    for copy in copies:
        copy.wait()
    layer_out[...] = kind(layer[...])
    low_out[...] = kind(low[...])[:, :4]
    high_out[...] = kind(high[...])[:, 4:]


def flag_ends(flags):
    xs, ys, nz = flags.shape
    layer, rows, few = ((ys, nz), (xs, 8, nz), (xs, 4, nz))
    return call(
        ends_kernel,
        [hbm()],
        [vmem()] * 3,
        [jax.ShapeDtypeStruct(a, I32) for a in (layer, few, few)],
        [pltpu.VMEM(a, I32) for a in (layer, rows, rows)] + [pltpu.SemaphoreType.DMA((3,))],
        limit=62,
        micros=1,
    )(flags)


def code_kernel(flags, tile, beyond, code):
    xs, zs = code.shape[0], code.shape[2] // LANES

    def encoded(x):
        def one(z):
            return jnp.concatenate([kind(flags[x, :, strip(z)]), tile[x, :, strip(z)]], 0)

        return [one(z) for z in range(zs)]

    def layer(x, e, e_next):
        o = [jnp.minimum(a, 1) for a in e]
        o_z = after_z(o)
        lane = lanes()
        o_z[-1] = jnp.where(lane == LANES - 1, 0, o_z[-1])
        for z in range(zs):
            c = o[z] & jnp.minimum(e_next[z], 1)
            c = c | ((o[z] & after_y(o[z])) << 1) | ((o[z] & o_z[z]) << 2)
            code[x, :, strip(z)] = c | jnp.where(e[z] == 2, LIQUID, 0)

    def step(x, carry):
        layer(x, encoded(x), encoded(x + 1))
        return carry

    lax.fori_loop(0, xs - 1, step, 0)
    layer(xs - 1, encoded(xs - 1), strips_of(beyond, (), zs))


def make_code(flags, tile, beyond):
    xs, _, nz = flags.shape
    return call(
        code_kernel, [vmem()] * 3, vmem(), jax.ShapeDtypeStruct((xs, ROWS, nz), I32)
    )(flags, tile, beyond)


def partial_spread(v, x, zs):
    vx, vy, vz = (strips_of(v, (a, x), zs) for a in range(3))
    vz_before = before_z(vz)
    return [vx[z] + (vy[z] - before_y(vy[z])) + (vz[z] - vz_before[z]) for z in range(zs)]


def send_layers(v, to_next, to_prior, xs, zs):
    for z, s in enumerate(partial_spread(v, 0, zs)):
        to_prior[:, strip(z)] = s
    to_next[...] = v[0, xs - 1]


def fill(read, code, guess, inverse, v, x, rows, z):
    at = (x, rows, strip(z))
    r = 1.0 / (read(3) + 1.0)
    inverse[at] = r
    bits = code[at]
    for a in range(3):
        g = read(a) * r
        guess[(a, *at)] = g
        v[(a, *at)] = jnp.where(bits & (1 << a) != 0, g, 0.0)


def fields_kernel(tot, code, guess, inverse, v):
    xs, ys, zs = code.shape[0], ROWS - 8, code.shape[2] // LANES

    def step(x, carry):
        for z in range(zs):
            for y in range(0, ys, 8):
                start = (x * ys + y) * COLUMN + z * 4
                read = lambda c: tot[pl.ds(start + c, 8, stride=COLUMN), :]
                fill(read, code, guess, inverse, v, x, slice(y, y + 8), z)
        return carry

    lax.fori_loop(0, xs, step, 0)


def fields(tot, code):
    xs, _, nz = code.shape
    one = jax.ShapeDtypeStruct((xs, ROWS, nz), F32)
    three = jax.ShapeDtypeStruct((3, xs, ROWS, nz), F32)
    return call(fields_kernel, [vmem()] * 2, [vmem()] * 3, [three, one, three])(tot, code)


def edge_kernel(after, prior, code, guess_in, inverse_in, v_in, guess, inverse, v, to_next, to_prior, edge):
    xs, ys, zs = code.shape[0], ROWS - 8, code.shape[2] // LANES
    for x in range(xs):
        edge[pl.ds(x * 256, 96), :] = after[pl.ds(x * 96, 96), :]
        edge[pl.ds(x * 256 + 96, 64), :] = jnp.zeros((64, LANES), F32)
        edge[pl.ds(x * 256 + 160, 96), :] = prior[pl.ds(x * 96, 96), :]

    def step(x, carry):
        for z in range(zs):
            read = lambda c: edge[pl.ds(x * 256 + z * 4 + c, 8, stride=32), :]
            fill(read, code, guess, inverse, v, x, slice(ys, ROWS), z)
        return carry

    lax.fori_loop(0, xs, step, 0)
    send_layers(v, to_next, to_prior, xs, zs)


def add_edge(after, prior, code, guess, inverse, v):
    xs, _, nz = code.shape
    layer = jax.ShapeDtypeStruct((ROWS, nz), F32)
    shapes = [jax.ShapeDtypeStruct(a.shape, F32) for a in (guess, inverse, v)]
    return call(
        edge_kernel,
        [vmem()] * 6,
        [vmem()] * 5,
        shapes + [layer, layer],
        [pltpu.VMEM((xs * 256, LANES), F32)],
        limit=4,
        micros=1,
        input_output_aliases={3: 0, 4: 1, 5: 2},
    )(after, prior, code, guess, inverse, v)


def ascend(p_out, p_in, v, code, x, before, first, zs):
    spread = partial_spread(v, x, zs)
    for z in range(zs):
        s = spread[z] - before(z)
        old = -STEP * s if first else p_in[x, :, strip(z)] - STEP * s
        liquid = code[x, :, strip(z)] & LIQUID != 0
        p_out[x, :, strip(z)] = jnp.where(liquid, jnp.maximum(old, 0.0), 0.0)


def push(v_out, p, code, guess, inverse, x, after, zs, axes=(0, 1, 2)):
    here = strips_of(p, (x,), zs)
    here_z = after_z(here) if 2 in axes else here
    for z in range(zs):
        r = inverse[x, :, strip(z)]
        bits = code[x, :, strip(z)]
        beyond = (after(z) if 0 in axes else None, after_y(here[z]), here_z[z])
        for a in axes:
            moved = guess[a, x, :, strip(z)] + (here[z] - beyond[a]) * r
            v_out[a, x, :, strip(z)] = jnp.where(bits & (1 << a) != 0, moved, 0.0)


def climb_inside(first, p_in, v_in, code, guess, inverse, p, v):
    xs, zs = code.shape[0], code.shape[2] // LANES

    def up(x, carry):
        ascend(p, p_in, v_in, code, x, lambda z: v_in[0, x - 1, :, strip(z)], first, zs)
        return carry

    lax.fori_loop(1, xs, up, 0)

    def out(x, carry):
        push(v, p, code, guess, inverse, x, lambda z: p[x + 1, :, strip(z)], zs)
        return carry

    lax.fori_loop(1, xs - 1, out, 0)
    push(v, p, code, guess, inverse, xs - 1, None, zs, (1, 2))


def climb_outside(first, before, spread, beyond, p8_in, p_in, v_in, code, guess, inverse, p, v, p8):
    xs, zs = code.shape[0], code.shape[2] // LANES
    ascend(p, p_in, v_in, code, 0, lambda z: before[:, strip(z)], first, zs)
    for z in range(zs):
        s = spread[:, strip(z)] - v_in[0, xs - 1, :, strip(z)]
        old = -STEP * s if first else p8_in[:, strip(z)] - STEP * s
        p8[:, strip(z)] = jnp.where(beyond[:, strip(z)] == 2, jnp.maximum(old, 0.0), 0.0)
    push(v, p, code, guess, inverse, 0, lambda z: p[1, :, strip(z)], zs)
    push(v, p, code, guess, inverse, xs - 1, lambda z: p8[:, strip(z)], zs, (0,))


def turn(v, guess, change, x, axes=(0, 1, 2)):
    ys, zs = ROWS - 8, v.shape[3] // LANES
    for a in axes:
        for z in range(zs):
            for y in range(0, ys, 8):
                at = (a, x, slice(y, y + 8), strip(z))
                change[pl.ds((x * ys + y) * COLUMN + z * 4 + a, 8, stride=COLUMN), :] = v[at] - guess[at]


def inner_first_kernel(v_in, code, guess, inverse, p, v):
    climb_inside(True, None, v_in, code, guess, inverse, p, v)


def inner_kernel(p_in, v_in, code, guess, inverse, p, v):
    climb_inside(False, p_in, v_in, code, guess, inverse, p, v)


def copy_pressure(p, p_out, x, sem):
    return pltpu.make_async_copy(p.at[x, pl.ds(0, ROWS - 8)], p_out.at[x], sem)


def copy_faces(v, v_out, a, x, sem):
    return pltpu.make_async_copy(v.at[a, x, pl.ds(0, ROWS - 8)], v_out.at[a, x], sem)


def inner_last_kernel(p_in, v_in, code, guess, inverse, p, v, change, p_out, v_out, sem):
    climb_inside(False, p_in, v_in, code, guess, inverse, p, v)
    xs = code.shape[0]

    def copies(x, axes):
        return [copy_pressure(p, p_out, x, sem.at[x])] + [copy_faces(v, v_out, a, x, sem.at[x]) for a in axes]

    for copy in copies(xs - 1, (1, 2)):
        copy.start()

    def step(x, carry):
        for copy in copies(x, (0, 1, 2)):
            copy.start()
        turn(v, guess, change, x)
        return carry

    lax.fori_loop(1, xs - 1, step, 0)
    turn(v, guess, change, xs - 1, (1, 2))
    for x in range(1, xs):
        for copy in copies(x, (0, 1, 2) if x < xs - 1 else (1, 2)):
            copy.wait()


def outer_first_kernel(before, spread, beyond, p_in, v_in, code, guess, inverse, p, v, p8, to_next, to_prior):
    climb_outside(True, before, spread, beyond, None, p_in, v_in, code, guess, inverse, p, v, p8)
    send_layers(v, to_next, to_prior, code.shape[0], code.shape[2] // LANES)


def outer_kernel(before, spread, beyond, p8_in, p_in, v_in, code, guess, inverse, p, v, p8, to_next, to_prior):
    climb_outside(False, before, spread, beyond, p8_in, p_in, v_in, code, guess, inverse, p, v, p8)
    send_layers(v, to_next, to_prior, code.shape[0], code.shape[2] // LANES)


def outer_last_kernel(
    before, spread, beyond, p8_in, names, change_in, p_in, v_in, code, guess, inverse, p_out_in, v_out_in,
    p, v, change, p_out, v_out, reply, p8, sem
):
    climb_outside(False, before, spread, beyond, p8_in, p_in, v_in, code, guess, inverse, p, v, p8)
    end = code.shape[0] - 1
    copies = [copy_pressure(p, p_out, 0, sem.at[0])]
    copies += [copy_faces(v, v_out, a, 0, sem.at[0]) for a in range(3)]
    copies.append(copy_faces(v, v_out, 0, end, sem.at[0]))
    for copy in copies:
        copy.start()
    turn(v, guess, change, 0)
    turn(v, guess, change, end, (0,))

    def step(g, carry):
        base = pl.multiple_of(g * 192, 192)
        for k in range(64):
            b = names[g * 64 + k]
            reply[pl.ds(base + 3 * k, 3), :] = change[pl.ds((b >> 3) * COLUMN + (b & 7) * 4, 3), :]
        return carry

    lax.fori_loop(0, reply.shape[0] // 192, step, 0)
    for copy in copies:
        copy.wait()


def like(*arrays):
    return [jax.ShapeDtypeStruct(a.shape, F32) for a in arrays]


def climb(names, v, code, guess, inverse, beyond, to_next, to_prior):
    xs, _, nz = code.shape
    rows = xs * (ROWS - 8) * COLUMN + 8
    for sweep in range(ITERS):
        before = shifted(to_next, "slab", 1)
        spread = shifted(to_prior, "slab", -1)
        rest = (code, guess, inverse)
        if sweep == 0:
            p, v = call(
                inner_first_kernel, [vmem()] * 4, [vmem()] * 2, like(inverse, v), input_output_aliases={0: 1}
            )(v, *rest)
            p, v, p8, to_next, to_prior = call(
                outer_first_kernel,
                [vmem()] * 8,
                [vmem()] * 5,
                like(p, v, before, before, before),
                micros=1,
                input_output_aliases={3: 0, 4: 1},
            )(before, spread, beyond, p, v, *rest)
        elif sweep < ITERS - 1:
            p, v = call(
                inner_kernel, [vmem()] * 5, [vmem()] * 2, like(p, v), input_output_aliases={0: 0, 1: 1}
            )(p, v, *rest)
            p, v, p8, to_next, to_prior = call(
                outer_kernel,
                [vmem()] * 9,
                [vmem()] * 5,
                like(p, v, before, before, before),
                micros=1,
                input_output_aliases={4: 0, 5: 1},
            )(before, spread, beyond, p8, p, v, *rest)
        else:
            change = jax.ShapeDtypeStruct((rows, LANES), F32)
            p_out = jax.ShapeDtypeStruct((xs, ROWS - 8, nz), F32)
            v_out = jax.ShapeDtypeStruct((3, xs, ROWS - 8, nz), F32)
            p, v, change, p_out, v_out = call(
                inner_last_kernel,
                [vmem()] * 5,
                [vmem()] * 3 + [hbm()] * 2,
                like(p, v) + [change, p_out, v_out],
                [pltpu.SemaphoreType.DMA((xs,))],
                micros=5,
                input_output_aliases={0: 0, 1: 1},
            )(p, v, *rest)
            reply = jax.ShapeDtypeStruct((names.shape[0] * 3, LANES), F32)
            p, v, change, p_out, v_out, reply = call(
                outer_last_kernel,
                [vmem()] * 4 + [smem()] + [vmem()] * 6 + [hbm()] * 2,
                [vmem()] * 3 + [hbm()] * 2 + [vmem()],
                like(p, v, change, p_out, v_out) + [reply],
                [
                    pltpu.VMEM(before.shape, F32),
                    pltpu.SemaphoreType.DMA((1,)),
                ],
                input_output_aliases={5: 2, 6: 0, 7: 1, 11: 3, 12: 4},
            )(before, spread, beyond, p8, names, change, p, v, *rest, p_out, v_out)
    return p_out, v_out, reply


def shifted(block, axis, distance):
    devices = range(lax.axis_size(axis))
    return lax.ppermute(block, axis, [(i - distance, i) for i in devices if i - distance in devices])


ITERS = 3


def on_device(velocity, weight, offset, owner, brick, flags):
    devices = lax.axis_size("slab") * lax.axis_size("sub")
    xs, ys, _ = flags.shape
    both = ("slab", "sub")
    layer, low, high = flag_ends(flags)
    beyond_own = shifted(layer, "slab", -1)
    later = shifted(low, "sub", -1)
    prior = shifted(high, "sub", 1)
    planes = velocity.transpose(1, 0, 2)
    outgoing, place = splat(planes, weight, offset, owner[:, 0], brick[:, 0], devices)
    tile = jnp.concatenate([later, prior], 1)
    beyond_edge = shifted(tile[0], "slab", -1)
    arrived = lax.all_to_all(outgoing.reshape(devices, 1, CHUNK * LANES), both, 0, 0, tiled=True)
    arrived, tile = lax.optimization_barrier((arrived, tile))
    names = arrived[:, 0, 32 * LANES : 32 * LANES + 8].astype(I32).reshape(-1)
    totals, first_rows, last_rows = scatter(arrived.reshape(devices * CHUNK, LANES), names, xs, ys)
    after = shifted(first_rows, "sub", -1)
    before = shifted(last_rows, "sub", 1)
    totals, tile, beyond_own, beyond_edge = lax.optimization_barrier((totals, tile, beyond_own, beyond_edge))
    beyond = jnp.concatenate([beyond_own, beyond_edge], 0)
    code = make_code(flags, tile, beyond)
    guess, inverse, v = fields(totals, code)
    guess, inverse, v, to_next, to_prior = add_edge(after, before, code, guess, inverse, v)
    p, v, reply = climb(names, v, code, guess, inverse, beyond, to_next, to_prior)
    back = lax.all_to_all(reply.reshape(devices, 24, LANES), both, 0, 0, tiled=True)
    updated = pick(back.reshape(devices * 24, LANES), planes, offset, place)
    return updated.transpose(1, 0, 2), p, v


def solution(mesh):
    return jax.shard_map(
        on_device,
        mesh=mesh,
        in_specs=(P(("slab", "sub")),) * 5 + (P("slab", "sub"),),
        out_specs=(P(("slab", "sub")), P("slab", "sub"), P(None, "slab", "sub")),
        check_vma=False,
    )
```

```python
import jax
import jax.numpy as jnp
from jax import lax
from jax.experimental import pallas as pl
from jax.experimental.pallas import tpu as pltpu
from jax.sharding import PartitionSpec as P

F32 = jnp.float32
BF16 = jnp.bfloat16
I32 = jnp.int32
LANES = 128
CHUNK = 33
COLUMN = 33
MIB = 1 << 20
GROUP = 128


def vmem():
    return pl.BlockSpec(memory_space=pltpu.VMEM)


def hbm():
    return pl.BlockSpec(memory_space=pltpu.HBM)


def smem():
    return pl.BlockSpec(memory_space=pltpu.SMEM)


def call(kernel, ins, outs, shapes, scratch=(), limit=3, micros=3, **kw):
    return pl.pallas_call(
        kernel,
        in_specs=ins,
        out_specs=outs,
        out_shape=shapes,
        scratch_shapes=list(scratch),
        compiler_params=pltpu.CompilerParams(vmem_limit_bytes=limit * MIB),
        cost_estimate=pl.CostEstimate(flops=micros * 100_000_000, bytes_accessed=1 << 20, transcendentals=0),
        **kw,
    )


def two_parts(x):
    high = x.astype(BF16).astype(F32)
    return high, x - high


def one_hot(offsets, cells):
    return jnp.where(jnp.broadcast_to(offsets, cells.shape) == cells, 1.0, 0.0).astype(BF16)


def splat_kernel(
    vel_hbm, weight_hbm, offset_hbm, owner_hbm, brick_hbm, out, place,
    vel, weight, offset, owner, brick, parts, names, count, sems
):
    pairs = ((vel_hbm, vel), (weight_hbm, weight), (offset_hbm, offset), (owner_hbm, owner), (brick_hbm, brick))
    copies = [pltpu.make_async_copy(a, b, sems.at[i]) for i, (a, b) in enumerate(pairs)]
    for copy in copies:
        copy.start()
    blocks = weight.shape[0]
    devices = names.shape[0]
    names[...] = jnp.full(names.shape, 4096.0, F32)

    def clear(g, carry):
        out[pl.ds(pl.multiple_of(g * 8, 8), 8), :] = jnp.zeros((8, LANES), F32)
        return carry

    lax.fori_loop(0, out.shape[0] // 8, clear, 0, unroll=16)

    def reset(d, carry):
        count[d] = 0
        return carry

    lax.fori_loop(0, devices, reset, 0, unroll=8)
    for copy in copies:
        copy.wait()

    def load(g, carry):
        for half in range(2):
            rows = pl.ds(pl.multiple_of(g * 16 + 8 * half, 8), 8)
            w = weight[rows, :]
            base = pl.multiple_of(g * 128, 128) + 4 * half
            for c in range(4):
                high, low = two_parts(vel[c, rows, :] * w if c < 3 else w)
                parts[pl.ds(base + c, 8, stride=16), :] = high
                parts[pl.ds(base + 8 + c, 8, stride=16), :] = low
        return carry

    lax.fori_loop(0, blocks // 16, load, 0, unroll=2)
    cells = lax.broadcasted_iota(I32, (LANES, LANES), 0)
    lane = lax.broadcasted_iota(I32, (1, LANES), 1)
    upper = lax.broadcasted_iota(I32, (16, LANES), 0) % 8 < 4

    def step(g, carry):
        base = pl.multiple_of(g * GROUP, GROUP)
        offs = offset[pl.ds(base, GROUP), :]
        sums = [None] * GROUP
        for t in range(GROUP // 16):
            for q in range(8):
                one, two = t * 16 + q, t * 16 + 8 + q
                hot = jnp.concatenate(
                    [one_hot(offs[one : one + 1, :], cells), one_hot(offs[two : two + 1, :], cells)], 1
                )
                x = parts[pl.ds(pl.multiple_of(base * 8, 8 * GROUP) + 128 * t + 16 * q, 16), :]
                lhs = jnp.concatenate([jnp.where(upper, x, 0.0), jnp.where(upper, 0.0, x)], 1).astype(BF16)
                r = lax.dot_general(lhs, hot, (((1,), (1,)), ((), ())), preferred_element_type=F32)
                r = r[0:8] + r[8:16]
                sums[one], sums[two] = r[0:4], r[4:8]
        for j in range(GROUP):
            d = owner[base + j]
            slot = count[d]
            count[d] = slot + 1
            place[base + j] = d * 8 + slot
            out[pl.ds(d * CHUNK + slot * 4, 4), :] = sums[j]
            b = brick[base + j]
            old = names[pl.ds(d, 1), :]
            names[pl.ds(d, 1), :] = jnp.where(lane == slot, jnp.full((1, LANES), b, I32).astype(F32), old)
        return carry

    lax.fori_loop(0, blocks // GROUP, step, 0)
    out[pl.ds(32, devices, stride=CHUNK), :] = names[...]


def splat(vel, weight, offset, owner, brick, devices):
    blocks = weight.shape[0]
    return call(
        splat_kernel,
        [hbm()] * 5,
        [vmem(), smem()],
        [jax.ShapeDtypeStruct((devices * CHUNK, LANES), F32), jax.ShapeDtypeStruct((blocks,), I32)],
        [
            pltpu.VMEM(vel.shape, F32),
            pltpu.VMEM(weight.shape, F32),
            pltpu.VMEM(offset.shape, I32),
            pltpu.SMEM((blocks,), I32),
            pltpu.SMEM((blocks,), I32),
            pltpu.VMEM((blocks * 8, LANES), F32),
            pltpu.VMEM((devices, LANES), F32),
            pltpu.SMEM((devices,), I32),
            pltpu.SemaphoreType.DMA((5,)),
        ],
        limit=60,
        micros=8,
    )(vel, weight, offset, owner, brick)


def pick_kernel(ret, vel, offset, place, out, parts, sums):
    blocks = offset.shape[0]
    cells = lax.broadcasted_iota(I32, (LANES, LANES), 0)
    upper = lax.broadcasted_iota(I32, (8, LANES), 0) < 4

    def gather(g, carry):
        base = pl.multiple_of(g * 16, 16)
        for j in range(16):
            high, low = two_parts(ret[pl.ds(place[base + j] * 3, 3), :])
            at = pl.multiple_of(base * 8, 128) + 16 * (j % 8) + 4 * (j // 8)
            parts[pl.ds(at, 3), :] = high
            parts[pl.ds(at + 8, 3), :] = low
        return carry

    lax.fori_loop(0, blocks // 16, gather, 0)

    def step(g, carry):
        base = pl.multiple_of(g * GROUP, GROUP)
        offs = offset[pl.ds(base, GROUP), :]
        for t in range(GROUP // 16):
            for q in range(8):
                one, two = t * 16 + q, t * 16 + 8 + q
                hot = jnp.concatenate(
                    [one_hot(offs[one : one + 1, :], cells), one_hot(offs[two : two + 1, :], cells)], 1
                )
                lhs = parts[pl.ds(pl.multiple_of(base * 8, 8 * GROUP) + 128 * t + 16 * q, 16), :].astype(BF16)
                r = lax.dot_general(lhs, hot, (((1,), (0,)), ((), ())), preferred_element_type=F32)
                r = r[0:8] + r[8:16]
                at = pl.multiple_of(base * 4, 4 * GROUP) + 64 * t + 8 * q
                sums[pl.ds(at, 8), :] = jnp.where(upper, r[:, :LANES], r[:, LANES:])
        return carry

    lax.fori_loop(0, blocks // GROUP, step, 0)

    def add(g, carry):
        for half in range(2):
            rows = pl.ds(pl.multiple_of(g * 16 + 8 * half, 8), 8)
            for c in range(3):
                change = sums[pl.ds(pl.multiple_of(g * 64, 64) + 4 * half + c, 8, stride=8), :]
                out[c, rows, :] = vel[c, rows, :] + change
        return carry

    lax.fori_loop(0, blocks // 16, add, 0, unroll=4)


def pick(ret, vel, offset, place):
    blocks = offset.shape[0]
    return call(
        pick_kernel,
        [vmem()] * 3 + [smem()],
        vmem(),
        jax.ShapeDtypeStruct((3, blocks, LANES), F32),
        [pltpu.VMEM((blocks * 8, LANES), F32), pltpu.VMEM((blocks * 4, LANES), F32)],
        limit=12,
        micros=6,
    )(ret, vel, offset, place)


def scatter_kernel(arr_hbm, names, tot, first, last, arr, sem):
    xs, ys = first.shape[0] // 96, 64
    per = 8 * CHUNK
    load = pltpu.make_async_copy(arr_hbm, arr, sem.at[0])
    load.start()

    def clear(g, carry):
        tot[pl.ds(pl.multiple_of(g * 8, 8), 8), :] = jnp.zeros((8, LANES), F32)
        return carry

    lax.fori_loop(0, tot.shape[0] // 8, clear, 0, unroll=16)
    load.wait()

    def step(g, carry):
        base = pl.multiple_of(g * per, 8)
        for first_slot in range(0, 64, 4):
            slots = range(first_slot, first_slot + 4)
            rows = []
            for k in slots:
                b = names[g * 64 + k]
                rows.append((b >> 3) * COLUMN + (b & 7) * 4)
            old = [tot[pl.ds(row, 4), :] for row in rows]
            new = [arr[pl.ds(base + (k // 8) * CHUNK + (k % 8) * 4, 4), :] for k in slots]
            for i in range(4):
                total = old[i] + new[i]
                for j in range(i):
                    total = total + jnp.where(rows[j] == rows[i], new[j], 0.0)
                tot[pl.ds(rows[i], 4), :] = total
        return carry

    lax.fori_loop(0, arr.shape[0] // per, step, 0)
    for x in range(xs):
        for r in range(3):
            first[pl.ds(x * 96 + r * 32, 32), :] = tot[pl.ds((x * ys + r) * COLUMN, 32), :]
            last[pl.ds(x * 96 + r * 32, 32), :] = tot[pl.ds((x * ys + ys - 3 + r) * COLUMN, 32), :]


def scatter(arr, names, xs, ys):
    rows = xs * ys * COLUMN + 8
    halo = jax.ShapeDtypeStruct((xs * 96, LANES), F32)
    return call(
        scatter_kernel,
        [hbm(), smem()],
        [vmem()] * 3,
        [jax.ShapeDtypeStruct((rows, LANES), F32), halo, halo],
        [pltpu.VMEM(arr.shape, F32), pltpu.SemaphoreType.DMA((1,))],
    )(arr, names)


ROWS = 72
LIQUID = 8
STEP = 0.15


def strip(z):
    return pl.ds(z * LANES, LANES)


def lanes():
    return lax.broadcasted_iota(I32, (ROWS, LANES), 1)


def before_y(a):
    return pltpu.roll(a, 1, 0)


def after_y(a):
    return pltpu.roll(a, ROWS - 1, 0)


def before_z(strips):
    lane = lanes()
    rolled = [pltpu.roll(a, 1, 1) for a in strips]
    return [jnp.where(lane == 0, rolled[z - 1], rolled[z]) for z in range(len(strips))]


def after_z(strips):
    lane = lanes()
    rolled = [pltpu.roll(a, LANES - 1, 1) for a in strips]
    last = len(strips) - 1
    return [jnp.where(lane == LANES - 1, rolled[z + 1 if z < last else 0], rolled[z]) for z in range(len(strips))]


def strips_of(ref, index, count):
    return [ref[(*index, slice(None), strip(z))] for z in range(count)]


def kind(f):
    return jnp.where(f == 2, 0, f + 1)


def ends_kernel(flags, layer_out, low_out, high_out, layer, low, high, sems):
    ys = flags.shape[1]
    copies = [
        pltpu.make_async_copy(flags.at[0], layer, sems.at[0]),
        pltpu.make_async_copy(flags.at[:, pl.ds(0, 8)], low, sems.at[1]),
        pltpu.make_async_copy(flags.at[:, pl.ds(ys - 8, 8)], high, sems.at[2]),
    ]
    for copy in copies:
        copy.start()
    for copy in copies:
        copy.wait()
    layer_out[...] = kind(layer[...])
    low_out[...] = kind(low[...])[:, :4]
    high_out[...] = kind(high[...])[:, 4:]


def flag_ends(flags):
    xs, ys, nz = flags.shape
    layer, rows, few = ((ys, nz), (xs, 8, nz), (xs, 4, nz))
    return call(
        ends_kernel,
        [hbm()],
        [vmem()] * 3,
        [jax.ShapeDtypeStruct(a, I32) for a in (layer, few, few)],
        [pltpu.VMEM(a, I32) for a in (layer, rows, rows)] + [pltpu.SemaphoreType.DMA((3,))],
        limit=62,
        micros=1,
    )(flags)


def code_kernel(flags, tile, beyond, code):
    xs, zs = code.shape[0], code.shape[2] // LANES

    def encoded(x):
        def one(z):
            return jnp.concatenate([kind(flags[x, :, strip(z)]), tile[x, :, strip(z)]], 0)

        return [one(z) for z in range(zs)]

    def layer(x, e, e_next):
        o = [jnp.minimum(a, 1) for a in e]
        o_z = after_z(o)
        lane = lanes()
        o_z[-1] = jnp.where(lane == LANES - 1, 0, o_z[-1])
        for z in range(zs):
            c = o[z] & jnp.minimum(e_next[z], 1)
            c = c | ((o[z] & after_y(o[z])) << 1) | ((o[z] & o_z[z]) << 2)
            code[x, :, strip(z)] = c | jnp.where(e[z] == 2, LIQUID, 0)

    def step(x, carry):
        layer(x, encoded(x), encoded(x + 1))
        return carry

    lax.fori_loop(0, xs - 1, step, 0)
    closed = jnp.zeros((8, LANES), I32)
    layer(xs - 1, encoded(xs - 1), [jnp.concatenate([a, closed], 0) for a in strips_of(beyond, (), zs)])


def make_code(flags, tile, beyond):
    xs, _, nz = flags.shape
    return call(
        code_kernel, [vmem()] * 3, vmem(), jax.ShapeDtypeStruct((xs, ROWS, nz), I32)
    )(flags, tile, beyond)


def partial_spread(v, x, zs):
    vx, vy, vz = (strips_of(v, (a, x), zs) for a in range(3))
    vz_before = before_z(vz)
    return [vx[z] + (vy[z] - before_y(vy[z])) + (vz[z] - vz_before[z]) for z in range(zs)]


def send_layers(v, to_next, to_prior, xs, zs):
    for z, s in enumerate(partial_spread(v, 0, zs)):
        to_prior[:, strip(z)] = s
    to_next[...] = v[0, xs - 1]


def fill(read, code, guess, inverse, v, x, rows, z):
    at = (x, rows, strip(z))
    r = 1.0 / (read(3) + 1.0)
    inverse[at] = r
    bits = code[at]
    for a in range(3):
        g = read(a) * r
        guess[(a, *at)] = g
        v[(a, *at)] = jnp.where(bits & (1 << a) != 0, g, 0.0)


def fields_kernel(tot, code, guess, inverse, v):
    xs, ys, zs = code.shape[0], ROWS - 8, code.shape[2] // LANES

    def step(x, carry):
        for z in range(zs):
            for y in range(0, ys, 8):
                start = (x * ys + y) * COLUMN + z * 4
                read = lambda c: tot[pl.ds(start + c, 8, stride=COLUMN), :]
                fill(read, code, guess, inverse, v, x, slice(y, y + 8), z)
        return carry

    lax.fori_loop(0, xs, step, 0)


def fields(tot, code):
    xs, _, nz = code.shape
    one = jax.ShapeDtypeStruct((xs, ROWS, nz), F32)
    three = jax.ShapeDtypeStruct((3, xs, ROWS, nz), F32)
    return call(fields_kernel, [vmem()] * 2, [vmem()] * 3, [three, one, three])(tot, code)


def edge_kernel(
    after, prior, tile, beyond, code_in, guess_in, inverse_in, v_in, code, guess, inverse, v, to_next, to_prior, edge
):
    xs, ys, zs = code.shape[0], ROWS - 8, code.shape[2] // LANES
    face_x = jnp.minimum(tile[xs - 1], 1) & jnp.minimum(beyond[...], 1)
    code[xs - 1, ys:ROWS] = code_in[xs - 1, ys:ROWS] | face_x
    for x in range(xs):
        edge[pl.ds(x * 256, 96), :] = after[pl.ds(x * 96, 96), :]
        edge[pl.ds(x * 256 + 96, 64), :] = jnp.zeros((64, LANES), F32)
        edge[pl.ds(x * 256 + 160, 96), :] = prior[pl.ds(x * 96, 96), :]

    def step(x, carry):
        for z in range(zs):
            read = lambda c: edge[pl.ds(x * 256 + z * 4 + c, 8, stride=32), :]
            fill(read, code, guess, inverse, v, x, slice(ys, ROWS), z)
        return carry

    lax.fori_loop(0, xs, step, 0)
    send_layers(v, to_next, to_prior, xs, zs)


def add_edge(after, prior, tile, beyond, code, guess, inverse, v):
    xs, _, nz = code.shape
    layer = jax.ShapeDtypeStruct((ROWS, nz), F32)
    shapes = [jax.ShapeDtypeStruct(a.shape, F32) for a in (guess, inverse, v)]
    return call(
        edge_kernel,
        [vmem()] * 8,
        [vmem()] * 6,
        [jax.ShapeDtypeStruct(code.shape, I32)] + shapes + [layer, layer],
        [pltpu.VMEM((xs * 256, LANES), F32)],
        limit=4,
        micros=1,
        input_output_aliases={4: 0, 5: 1, 6: 2, 7: 3},
    )(after, prior, tile, beyond, code, guess, inverse, v)


def ascend(p_out, p_in, v, code, x, before, first, zs):
    spread = partial_spread(v, x, zs)
    for z in range(zs):
        s = spread[z] - before(z)
        old = -STEP * s if first else p_in[x, :, strip(z)] - STEP * s
        liquid = code[x, :, strip(z)] & LIQUID != 0
        p_out[x, :, strip(z)] = jnp.where(liquid, jnp.maximum(old, 0.0), 0.0)


def push(v_out, p, code, guess, inverse, x, after, zs, axes=(0, 1, 2)):
    here = strips_of(p, (x,), zs)
    here_z = after_z(here) if 2 in axes else here
    for z in range(zs):
        r = inverse[x, :, strip(z)]
        bits = code[x, :, strip(z)]
        beyond = (after(z) if 0 in axes else None, after_y(here[z]), here_z[z])
        for a in axes:
            moved = guess[a, x, :, strip(z)] + (here[z] - beyond[a]) * r
            v_out[a, x, :, strip(z)] = jnp.where(bits & (1 << a) != 0, moved, 0.0)


def climb_inside(first, p_in, v_in, code, guess, inverse, p, v):
    xs, zs = code.shape[0], code.shape[2] // LANES

    def up(x, carry):
        ascend(p, p_in, v_in, code, x, lambda z: v_in[0, x - 1, :, strip(z)], first, zs)
        return carry

    lax.fori_loop(1, xs, up, 0)

    def out(x, carry):
        push(v, p, code, guess, inverse, x, lambda z: p[x + 1, :, strip(z)], zs)
        return carry

    lax.fori_loop(1, xs - 1, out, 0)
    push(v, p, code, guess, inverse, xs - 1, None, zs, (1, 2))


def climb_outside(first, before, spread, beyond, p8_in, p_in, v_in, code, guess, inverse, p, v, p8):
    xs, zs = code.shape[0], code.shape[2] // LANES
    ascend(p, p_in, v_in, code, 0, lambda z: before[:, strip(z)], first, zs)
    for z in range(zs):
        s = spread[:, strip(z)] - v_in[0, xs - 1, :, strip(z)]
        old = -STEP * s if first else p8_in[:, strip(z)] - STEP * s
        p8[:, strip(z)] = jnp.where(beyond[:, strip(z)] == 2, jnp.maximum(old, 0.0), 0.0)
    push(v, p, code, guess, inverse, 0, lambda z: p[1, :, strip(z)], zs)
    push(v, p, code, guess, inverse, xs - 1, lambda z: p8[:, strip(z)], zs, (0,))


def turn(v, guess, change, x, axes=(0, 1, 2)):
    ys, zs = ROWS - 8, v.shape[3] // LANES
    for a in axes:
        for z in range(zs):
            for y in range(0, ys, 8):
                at = (a, x, slice(y, y + 8), strip(z))
                change[pl.ds((x * ys + y) * COLUMN + z * 4 + a, 8, stride=COLUMN), :] = v[at] - guess[at]


def inner_first_kernel(v_in, code, guess, inverse, p, v):
    climb_inside(True, None, v_in, code, guess, inverse, p, v)


def inner_kernel(p_in, v_in, code, guess, inverse, p, v):
    climb_inside(False, p_in, v_in, code, guess, inverse, p, v)


def copy_pressure(p, p_out, x, sem):
    return pltpu.make_async_copy(p.at[x, pl.ds(0, ROWS - 8)], p_out.at[x], sem)


def copy_faces(v, v_out, a, x, sem):
    return pltpu.make_async_copy(v.at[a, x, pl.ds(0, ROWS - 8)], v_out.at[a, x], sem)


def inner_last_kernel(p_in, v_in, code, guess, inverse, p, v, change, p_out, v_out, sem):
    climb_inside(False, p_in, v_in, code, guess, inverse, p, v)
    xs = code.shape[0]

    def copies(x, axes):
        return [copy_pressure(p, p_out, x, sem.at[x])] + [copy_faces(v, v_out, a, x, sem.at[x]) for a in axes]

    for copy in copies(xs - 1, (1, 2)):
        copy.start()

    def step(x, carry):
        for copy in copies(x, (0, 1, 2)):
            copy.start()
        turn(v, guess, change, x)
        return carry

    lax.fori_loop(1, xs - 1, step, 0)
    turn(v, guess, change, xs - 1, (1, 2))
    for x in range(1, xs):
        for copy in copies(x, (0, 1, 2) if x < xs - 1 else (1, 2)):
            copy.wait()


def outer_first_kernel(before, spread, beyond, p_in, v_in, code, guess, inverse, p, v, p8, to_next, to_prior):
    climb_outside(True, before, spread, beyond, None, p_in, v_in, code, guess, inverse, p, v, p8)
    send_layers(v, to_next, to_prior, code.shape[0], code.shape[2] // LANES)


def outer_kernel(before, spread, beyond, p8_in, p_in, v_in, code, guess, inverse, p, v, p8, to_next, to_prior):
    climb_outside(False, before, spread, beyond, p8_in, p_in, v_in, code, guess, inverse, p, v, p8)
    send_layers(v, to_next, to_prior, code.shape[0], code.shape[2] // LANES)


def outer_last_kernel(
    before, spread, beyond, p8_in, names, change_in, p_in, v_in, code, guess, inverse, p_out_in, v_out_in,
    p, v, change, p_out, v_out, reply, p8, sem
):
    climb_outside(False, before, spread, beyond, p8_in, p_in, v_in, code, guess, inverse, p, v, p8)
    end = code.shape[0] - 1
    copies = [copy_pressure(p, p_out, 0, sem.at[0])]
    copies += [copy_faces(v, v_out, a, 0, sem.at[0]) for a in range(3)]
    copies.append(copy_faces(v, v_out, 0, end, sem.at[0]))
    for copy in copies:
        copy.start()
    turn(v, guess, change, 0)
    turn(v, guess, change, end, (0,))

    def step(g, carry):
        base = pl.multiple_of(g * 192, 192)
        for k in range(64):
            b = names[g * 64 + k]
            reply[pl.ds(base + 3 * k, 3), :] = change[pl.ds((b >> 3) * COLUMN + (b & 7) * 4, 3), :]
        return carry

    lax.fori_loop(0, reply.shape[0] // 192, step, 0)
    for copy in copies:
        copy.wait()


def like(*arrays):
    return [jax.ShapeDtypeStruct(a.shape, F32) for a in arrays]


def climb(names, v, code, guess, inverse, beyond, to_next, to_prior):
    xs, _, nz = code.shape
    rows = xs * (ROWS - 8) * COLUMN + 8
    for sweep in range(ITERS):
        before = shifted(to_next, "slab", 1)
        spread = shifted(to_prior, "slab", -1)
        rest = (code, guess, inverse)
        if sweep == 0:
            p, v = call(
                inner_first_kernel, [vmem()] * 4, [vmem()] * 2, like(inverse, v), input_output_aliases={0: 1}
            )(v, *rest)
            p, v, p8, to_next, to_prior = call(
                outer_first_kernel,
                [vmem()] * 8,
                [vmem()] * 5,
                like(p, v, before, before, before),
                micros=1,
                input_output_aliases={3: 0, 4: 1},
            )(before, spread, beyond, p, v, *rest)
        elif sweep < ITERS - 1:
            p, v = call(
                inner_kernel, [vmem()] * 5, [vmem()] * 2, like(p, v), input_output_aliases={0: 0, 1: 1}
            )(p, v, *rest)
            p, v, p8, to_next, to_prior = call(
                outer_kernel,
                [vmem()] * 9,
                [vmem()] * 5,
                like(p, v, before, before, before),
                micros=1,
                input_output_aliases={4: 0, 5: 1},
            )(before, spread, beyond, p8, p, v, *rest)
        else:
            change = jax.ShapeDtypeStruct((rows, LANES), F32)
            p_out = jax.ShapeDtypeStruct((xs, ROWS - 8, nz), F32)
            v_out = jax.ShapeDtypeStruct((3, xs, ROWS - 8, nz), F32)
            p, v, change, p_out, v_out = call(
                inner_last_kernel,
                [vmem()] * 5,
                [vmem()] * 3 + [hbm()] * 2,
                like(p, v) + [change, p_out, v_out],
                [pltpu.SemaphoreType.DMA((xs,))],
                micros=5,
                input_output_aliases={0: 0, 1: 1},
            )(p, v, *rest)
            reply = jax.ShapeDtypeStruct((names.shape[0] * 3, LANES), F32)
            p, v, change, p_out, v_out, reply = call(
                outer_last_kernel,
                [vmem()] * 4 + [smem()] + [vmem()] * 6 + [hbm()] * 2,
                [vmem()] * 3 + [hbm()] * 2 + [vmem()],
                like(p, v, change, p_out, v_out) + [reply],
                [
                    pltpu.VMEM(before.shape, F32),
                    pltpu.SemaphoreType.DMA((1,)),
                ],
                input_output_aliases={5: 2, 6: 0, 7: 1, 11: 3, 12: 4},
            )(before, spread, beyond, p8, names, change, p, v, *rest, p_out, v_out)
    return p_out, v_out, reply


def shifted(block, axis, distance):
    devices = range(lax.axis_size(axis))
    return lax.ppermute(block, axis, [(i - distance, i) for i in devices if i - distance in devices])


ITERS = 3


def on_device(velocity, weight, offset, owner, brick, flags):
    devices = lax.axis_size("slab") * lax.axis_size("sub")
    xs, ys, _ = flags.shape
    both = ("slab", "sub")
    layer, low, high = flag_ends(flags)
    beyond_own = shifted(layer, "slab", -1)
    later = shifted(low, "sub", -1)
    prior = shifted(high, "sub", 1)
    planes = velocity.transpose(1, 0, 2)
    outgoing, place = splat(planes, weight, offset, owner[:, 0], brick[:, 0], devices)
    tile = jnp.concatenate([later, prior], 1)
    beyond_edge = shifted(tile[0], "slab", -1)
    arrived = lax.all_to_all(outgoing.reshape(devices, 1, CHUNK * LANES), both, 0, 0, tiled=True)
    arrived, tile, beyond_own = lax.optimization_barrier((arrived, tile, beyond_own))
    names = arrived[:, 0, 32 * LANES : 32 * LANES + 8].astype(I32).reshape(-1)
    totals, first_rows, last_rows = scatter(arrived.reshape(devices * CHUNK, LANES), names, xs, ys)
    after = shifted(first_rows, "sub", -1)
    before = shifted(last_rows, "sub", 1)
    totals, tile, beyond_own = lax.optimization_barrier((totals, tile, beyond_own))
    code = make_code(flags, tile, beyond_own)
    guess, inverse, v = fields(totals, code)
    code, guess, inverse, v, to_next, to_prior = add_edge(
        after, before, tile, beyond_edge, code, guess, inverse, v
    )
    beyond = jnp.concatenate([beyond_own, beyond_edge], 0)
    p, v, reply = climb(names, v, code, guess, inverse, beyond, to_next, to_prior)
    back = lax.all_to_all(reply.reshape(devices, 24, LANES), both, 0, 0, tiled=True)
    updated = pick(back.reshape(devices * 24, LANES), planes, offset, place)
    return updated.transpose(1, 0, 2), p, v


def solution(mesh):
    return jax.shard_map(
        on_device,
        mesh=mesh,
        in_specs=(P(("slab", "sub")),) * 5 + (P("slab", "sub"),),
        out_specs=(P(("slab", "sub")), P("slab", "sub"), P(None, "slab", "sub")),
        check_vma=False,
    )
```
